32 devices in a mesh: groups: 2 (over y), tmpl: 8 (over z, x), det: 2 (over core).
Axes of the slice: x: 2, y: 2, z: 4, core: 2. Of those that a mesh axis runs over, the one named last changes fastest.
Arguments:
- basis_series: bfloat16 [3, 128, 32768], P(None, None, ('groups', 'tmpl', 'det')), parts along dimension 2, may hold values from -6 to 6
- reconstruction: bfloat16 [3, 256, 2, 128], P(None, ('groups', 'tmpl')), parts along dimension 1, may hold values from -0.5 to 0.5
- offsets: int32 [6], P('groups'), parts along dimension 0, may hold values from 1024 to 16383
Outputs:
- window_peaks: float32 [128, 256], P(None, ('groups', 'tmpl', 'det')), parts along dimension 1
The draws below stay inside these ranges and needn't reach their ends.
There are 2 independent parts, one for each index of `groups`. The reference program is written for one: setup_inputs(seed, part) draws one part's arguments, and reference() takes and returns one part's arrays. A program takes and returns all parts, laid end to end along the dimension named above; each array names one. Nothing has to cross between parts.
Inputs may be any that keep to these rules, and one draw needn't show every extreme that they name: `offsets`: slides are applied circularly over the segment's 16384 samples.
All inputs are finite; a program needn't handle non-finite values.
Results may differ from the reference program's by a relative error of at most 0.0003.
Values may be sent and summed in bfloat16 or wider, within the bound.
A program may use at most 64 MiB of HBM per device.

```python
import jax
import jax.numpy as jnp
from jax import lax

DETS = 3
BASIS = 128
WIN = 128
T_DEV = 1024
MAXQ = 16
TEMPL = 128
NT = 16384
NWIN = 128


def level_of(key, dims, pieces, low, top_value):
    factor_of = 1.0
    for axis_at, shards_of in pieces:
        steps = jax.random.uniform(jax.random.fold_in(jax.random.fold_in(key, 6), axis_at), (shards_of,), jnp.float32, low / len(pieces), top_value / len(pieces))
        factor_of = factor_of * jnp.repeat(jnp.exp(steps), dims[axis_at] // shards_of).reshape((-1,) + (1,) * (len(dims) - 1 - axis_at))
    return factor_of


def bell_draw(key, shape, spread, limit, pieces=(), dtype=jnp.bfloat16):
    level = level_of(key, shape, pieces, -0.22, 0.18) if pieces else 1.0
    drawn = jax.random.normal(key, shape, jnp.float32) * spread * level
    return jnp.minimum(jnp.maximum(drawn, -limit), limit).astype(dtype)


def setup_inputs(seed: int = 0, part: int = 0) -> dict:
    key_of = jax.random.split(jax.random.key(seed), 4)
    part_keys = jax.random.split(jax.random.fold_in(key_of[3], part), 4)
    basis_series = bell_draw(part_keys[0], (DETS, BASIS, NT), 1.0, 6.0, ((2, 16),))
    reconstruction = bell_draw(part_keys[1], (DETS, TEMPL, 2, BASIS), BASIS ** -0.5, 0.5, ((1, 8),))
    offsets = jax.random.randint(part_keys[2], (DETS,), T_DEV, MAXQ * T_DEV).astype(jnp.int32)
    return dict(basis_series=basis_series, reconstruction=reconstruction, offsets=offsets)


def reference(basis_series, reconstruction, offsets):
    slid_series = jnp.stack([jnp.roll(basis_series[detector], -offsets[detector], axis=1) for detector in range(DETS)])
    block_count = NT // T_DEV
    blocks = slid_series.reshape(DETS, BASIS, block_count, T_DEV).transpose(2, 0, 1, 3)

    def one_block(block):
        power_sum = jnp.zeros((TEMPL, T_DEV), jnp.float32)
        for detector in range(DETS):
            filtered = jnp.dot(reconstruction[detector].reshape(2 * TEMPL, BASIS), block[detector], preferred_element_type=jnp.float32)
            filtered = filtered.reshape(TEMPL, 2, T_DEV)
            power_sum = power_sum + lax.optimization_barrier(jnp.sum(filtered * filtered, axis=1))
        network = jnp.sqrt(power_sum)
        return lax.optimization_barrier(jnp.max(network.reshape(TEMPL, T_DEV // WIN, WIN), axis=2))
    peaks = lax.map(one_block, blocks)
    return peaks.transpose(1, 0, 2).reshape(TEMPL, NWIN)
```

```python
import functools
import math

import jax
import jax.numpy as jnp
from jax import lax
from jax.experimental import pallas as pl
from jax.experimental.pallas import tpu as pltpu
from jax.sharding import PartitionSpec as P

WIN = 128
SUB = 8
SLIDE_BLOCKS = 16
MESH = pl.DeviceIdType.MESH
TINY = 1e-18
CODE = jnp.int16
SPAN = 30
STEPS = 1092
TOP = 15


def coded(power):
    log = jnp.log(jnp.maximum(power, 2.0 ** (TOP - 2 * SPAN))) * (STEPS / math.log(2.0))
    return jnp.round(log - (TOP - SPAN) * STEPS).astype(jnp.int32).astype(CODE)


def decoded(code):
    code = code.astype(jnp.int32).astype(jnp.float32)
    power = jnp.exp2(code * (1.0 / STEPS) + (TOP - SPAN))
    return jnp.where(code <= -SPAN * STEPS, 0.0, power)


def kernel(
    chips, cores,
    off_hbm, basis_hbm, bank_hbm, out_ref,
    off_ref, basis_ref, bank_ref, bank_own, bank_all, stage, recv, dec, peaks, final,
    load, bank_s, fwd_s, pass_s, bank_r, pow_s, pow_r, peak_s, peak_r,
):
    dets, basis, block = basis_ref.shape
    rows2 = bank_ref.shape[1] // cores
    rows = rows2 // 2
    half = block // 2
    wins = block // WIN
    count = chips * cores
    total = count * wins
    per_row = WIN // rows
    near = chips // 2
    chip, core = lax.axis_index("tmpl"), lax.axis_index("det")
    me = chip * cores + core
    side, place = lax.div(chip, near), lax.rem(chip, near)

    load_bank = pltpu.make_async_copy(bank_hbm, bank_ref, load.at[0])
    load_basis = pltpu.make_async_copy(basis_hbm, basis_ref, load.at[1])
    load_off = pltpu.make_async_copy(off_hbm, off_ref, load.at[2])
    load_bank.start()
    load_basis.start()
    load_off.start()

    def dev(j, c):
        return {"tmpl": j, "det": c}

    def across(j):
        return lax.rem(j + near, chips)

    def close(k):
        if near & (near - 1):
            return side * near + lax.rem(place + near + k, near)
        return side * near + lax.bitwise_xor(place, jnp.int32(k))

    def facing(k):
        return close(-k if near & (near - 1) else k)

    def other_core(d):
        return lax.rem(core + d, cores)

    def over(lo, hi, fn, short=True):
        if short and hi - lo <= 8:
            for k in range(lo, hi):
                fn(k)
            return

        @pl.loop(lo, hi)
        def _(k):
            fn(k)

    def over_peers(fn):
        for d in range(1, cores):
            fn(chip, other_core(d))
        for d in range(cores):
            c = other_core(d)
            over(0, near, lambda k: fn(across(close(k)), c))
            over(1, near, lambda k: fn(close(k), c))

    barrier = pltpu.get_barrier_semaphore()
    over_peers(lambda j, c: pl.semaphore_signal(barrier, inc=1, device_id=dev(j, c), device_id_type=MESH))

    def bank_copy(j, src, sem):
        return pltpu.make_async_remote_copy(
            src_ref=bank_all.at[src], dst_ref=bank_all.at[src], send_sem=sem, recv_sem=bank_r.at[src],
            device_id=dev(j, core), device_id_type=MESH)

    def pass_copy(src, c):
        return pltpu.make_async_remote_copy(
            src_ref=bank_all.at[src], dst_ref=bank_all.at[src],
            send_sem=pass_s.at[lax.div(src, cores) * cores + c], recv_sem=bank_r.at[src],
            device_id=dev(chip, c), device_id_type=MESH)

    def pow_copy(j, c, src):
        return pltpu.make_async_remote_copy(
            src_ref=stage.at[j * cores + c], dst_ref=recv.at[src],
            send_sem=pow_s.at[j * cores + c], recv_sem=pow_r.at[src],
            device_id=dev(j, c), device_id_type=MESH)

    def peak_row(j, c):
        i = j * cores + c
        return lax.div(i, per_row) * SUB + lax.rem(SUB - lax.rem(i, SUB), SUB)

    def peak_copy(j, c, src):
        return pltpu.make_async_remote_copy(
            src_ref=peaks.at[peak_row(j, c)], dst_ref=final.at[src],
            send_sem=peak_s.at[j * cores + c], recv_sem=peak_r.at[src],
            device_id=dev(j, c), device_id_type=MESH)

    span = dets * rows2
    size = span * cores
    r = lax.broadcasted_iota(jnp.int32, (size, size), 0)
    i = lax.broadcasted_iota(jnp.int32, (size, size), 1)
    c_of = lax.div(r, span)
    d_of = lax.rem(lax.div(r, rows2), dets)
    k_of = lax.rem(lax.div(r, rows), 2)
    m_of = lax.rem(r, rows)
    perm = (i == (d_of * cores + c_of) * rows2 + m_of * 2 + k_of).astype(jnp.float32).astype(jnp.bfloat16)

    def largest(x):
        x = jnp.abs(x).astype(jnp.float32)
        x = jnp.max(x.reshape(-1, SUB, x.shape[-1]), axis=0)
        return jnp.max(jnp.max(x, axis=0, keepdims=True), axis=1, keepdims=True)

    load_bank.wait()
    sorted_bank = jnp.dot(
        perm, bank_ref[...].reshape(size, basis), preferred_element_type=jnp.float32).astype(jnp.bfloat16)
    for c in range(cores):
        bank_own[c, :span] = sorted_bank[c * span:(c + 1) * span]
    load_basis.wait()
    top = largest(basis_ref[...].reshape(dets * basis, block))
    for c in range(cores):
        own_max = largest(sorted_bank[c * span:(c + 1) * span])
        note = jnp.concatenate([jnp.broadcast_to(top, (SUB, basis)), jnp.broadcast_to(own_max, (SUB, basis))], axis=0)
        bank_own[c, span:] = note.astype(jnp.bfloat16)
    bank_all[me] = bank_own[core]

    def bank_max(bank, src):
        return bank[src, span + SUB:].astype(jnp.float32)[:1, :1]

    def powers_for(j, bank, first):
        to = across(j)
        inv = []
        for c in range(cores):
            a = jnp.maximum(bank_max(bank, first + c) * top, TINY)
            inv.append(1.0 / (a * a))
        for d in range(dets):
            w = jnp.concatenate(
                [bank[first + c, d * rows2:(d + 1) * rows2] for c in range(cores)], axis=0)
            f = jnp.dot(w, basis_ref[d], preferred_element_type=jnp.float32)
            f = f * f
            for c in range(cores):
                p = (f[c * rows2:c * rows2 + rows] + f[c * rows2 + rows:(c + 1) * rows2]) * inv[c]
                stage[to * cores + c, d] = coded(jnp.concatenate([p[:, :half], p[:, half:]], axis=0))

    def pieces(j, fn):
        for d in range(1, cores):
            fn(j * cores + other_core(d))

    powers_for(chip, bank_own, 0)
    pl.semaphore_wait(barrier, count - 1)

    bank_copy(across(chip), me, bank_s.at[0]).start()
    over(1, near, lambda k: bank_copy(facing(k), me, bank_s.at[k]).start())
    for c in range(cores):
        pow_copy(across(chip), c, me).start()
    for d in range(1, cores):
        pass_copy(me, other_core(d)).start()

    def pass_on(src):
        bank_copy(chip, src, bank_s.at[0]).wait_recv()
        for d in range(1, cores):
            pass_copy(src, other_core(d)).start()

    over(1, near, lambda k: pass_on(close(k) * cores + core))
    relay = across(chip) * cores + core
    pass_on(relay)
    over(1, near, lambda k: bank_copy(facing(k), relay, fwd_s.at[k]).start())

    def near_powers(k):
        j = close(k)
        pieces(j, lambda src: bank_copy(chip, src, bank_s.at[0]).wait_recv())
        powers_for(j, bank_all, j * cores)
        for c in range(cores):
            pow_copy(across(j), c, me).start()

    over(1, near, near_powers, short=False)

    over(1, near, lambda k: pass_on(across(close(k)) * cores + core))
    pieces(across(chip), lambda src: bank_copy(chip, src, bank_s.at[0]).wait_recv())
    powers_for(across(chip), bank_all, across(chip) * cores)
    for d in range(1, cores):
        pow_copy(chip, other_core(d), me).start()

    def far_powers(k):
        j = across(close(k))
        pieces(j, lambda src: bank_copy(chip, src, bank_s.at[0]).wait_recv())
        powers_for(j, bank_all, j * cores)
        for c in range(cores):
            pow_copy(close(k), c, me).start()

    over(1, near, far_powers, short=False)

    load_off.wait()
    rest = [lax.rem(off_ref[d], WIN) for d in range(dets)]
    shifts = [lax.div(off_ref[d], WIN) for d in range(dets)]
    owned = bank_max(bank_all, across(chip) * cores + core)

    def decode(src, value):
        a = jnp.maximum(bank_all[src, span:span + SUB].astype(jnp.float32)[:1, :1] * owned, TINY)
        scale = a * a
        for d in range(dets):
            x = decoded(value(d)) * scale
            tiles = []
            for v in range(wins):
                h, q = divmod(v, wins // 2)
                tile = x[h * rows:(h + 1) * rows, q * WIN:(q + 1) * WIN]
                tile = pltpu.roll(tile, WIN - rest[d], 1)
                dec[d, src * wins + v] = tile
                tiles.append(tile)

            @pl.when(src < SLIDE_BLOCKS)
            def _():
                for v in range(wins):
                    dec[d, (count + src) * wins + v] = tiles[v]

    decode(me, lambda d: stage[me, d])

    def take(j, c):
        src = j * cores + c
        pow_copy(chip, core, src).wait_recv()
        decode(src, lambda d: recv[src, d])

    @pl.loop(0, cores)
    def _(c):
        take(across(chip), c)

    pieces(chip, lambda src: bank_copy(chip, src, bank_s.at[0]).wait_recv())
    for d in range(1, cores):
        take(chip, other_core(d))

    def take_pair(k):
        @pl.loop(0, 2 * cores)
        def _(n):
            far = lax.div(n, cores)
            j = lax.rem(facing(k) + far * near, chips)
            take(j, lax.rem(n, cores))

    over(1, near, take_pair, short=False)

    lane = lax.broadcasted_iota(jnp.int32, (rows, WIN), 1)
    inside = [lane < WIN - rest[d] for d in range(dets)]
    bit = [lax.rem(lax.div(lane, 1 << p), 2) == 0 for p in range(7)]
    row = lax.broadcasted_iota(jnp.int32, (rows, WIN), 0)
    dest = lax.rem(SUB - row, SUB) + SUB * lax.div(lane, WIN // 2)
    index = SUB * lax.rem(dest + lax.rem(lane, SUB), per_row) + lax.rem(lax.div(lane, SUB), SUB)

    def group(g):
        base = g * WIN
        last = {}

        def tile(d, v):
            if last.get(d, (None, None))[0] != v:
                last[d] = (v, dec[d, base + shifts[d] + v])
            return last[d][1]

        def leaf(v):
            power = None
            for d in range(dets):
                lo = tile(d, v)
                x = jnp.where(inside[d], lo, tile(d, v + 1))
                power = x if power is None else power + x
            return power

        def merged(k, v):
            if k == 0:
                return leaf(v)
            p = k - 1
            a = merged(p, v)
            b = merged(p, v + (1 << p))
            s = jnp.where(bit[p], a, b)
            t = jnp.where(bit[p], b, a)
            return jnp.maximum(s, pltpu.roll(t, WIN - (1 << p), 1))

        x = jnp.sqrt(merged(7, 0))
        x = pltpu.roll(x, 0, 1, stride=SUB, stride_axis=0)
        for p in range(3):
            x = jnp.where(bit[3 + p], x, pltpu.roll(x, SUB - (1 << p), 0))
        x = jnp.take_along_axis(x, index, axis=1)
        for s in range(SUB):
            peaks[g * SUB + s] = x[s:s + 1]

    over(0, total // WIN, group, short=total == WIN)

    over_peers(lambda j, c: peak_copy(j, c, me).start())
    final[me] = peaks[peak_row(chip, core)]
    over_peers(lambda j, c: peak_copy(chip, core, j * cores + c).wait_recv())

    high = lax.rem(lax.div(me, SUB), 2) * (WIN // 2)
    e_of = lax.broadcasted_iota(jnp.int32, (per_row, WIN), 0)
    l_of = lax.broadcasted_iota(jnp.int32, (per_row, WIN), 1)
    groups = count // per_row
    for g in range(groups):
        to = (g + groups // 2) % groups if groups > 1 else 0
        x = final[g * per_row:(g + 1) * per_row].reshape(per_row, WIN)
        x = pltpu.roll(x, lax.rem(WIN - high, WIN), 1)
        turn = 0 if groups > 1 else per_row // 2
        x = jnp.concatenate([
            pltpu.roll(x[h:h + SUB], (h + turn) * rows % WIN, 1, stride=rows, stride_axis=0)
            for h in range(0, per_row, SUB)], axis=0)
        for i in range(wins):
            y = pltpu.roll(x, (WIN - i * rows) % WIN, 1)
            y = jnp.where(lax.div(l_of, rows) == lax.rem(e_of + turn, per_row), y, 0.0)
            out_ref[i:i + 1, to * WIN:(to + 1) * WIN] = jnp.sum(y, axis=0, keepdims=True)

    bank_copy(across(chip), me, bank_s.at[0]).wait_send()
    over(1, near, lambda k: bank_copy(facing(k), me, bank_s.at[k]).wait_send())
    over(1, near, lambda k: bank_copy(facing(k), relay, fwd_s.at[k]).wait_send())

    def passed(j):
        for d in range(1, cores):
            pass_copy(j * cores + core, other_core(d)).wait_send()

    over(0, near, lambda k: passed(close(k)))
    over(0, near, lambda k: passed(across(close(k))))

    def drain(j, c):
        pow_copy(j, c, me).wait_send()
        peak_copy(j, c, me).wait_send()

    over_peers(drain)


def per_device(chips, cores, basis_series, reconstruction, offsets):
    dets, basis, block = basis_series.shape
    templates = reconstruction.shape[1]
    bank = reconstruction.reshape(dets, templates * 2, basis)
    count = chips * cores
    rows = templates // cores
    wins = block // WIN
    total = count * wins
    hbm = pl.BlockSpec(memory_space=pltpu.HBM)
    scratch = [
        pltpu.SMEM(offsets.shape, offsets.dtype),
        pltpu.VMEM(basis_series.shape, basis_series.dtype),
        pltpu.VMEM(bank.shape, bank.dtype),
        pltpu.VMEM((cores, dets * rows * 2 + 2 * SUB, basis), jnp.bfloat16),
        pltpu.VMEM((count, dets * rows * 2 + 2 * SUB, basis), jnp.bfloat16),
        pltpu.VMEM((count, dets, rows * 2, block // 2), CODE),
        pltpu.VMEM((count, dets, rows * 2, block // 2), CODE),
        pltpu.VMEM((dets, total + SLIDE_BLOCKS * wins, rows, WIN), jnp.float32),
        pltpu.VMEM((total // WIN * SUB, 1, WIN), jnp.float32),
        pltpu.VMEM((count, 1, WIN), jnp.float32),
    ]
    held = sum(math.prod(x.shape) * jnp.dtype(x.dtype).itemsize for x in scratch[1:-2])
    held += (count + total // WIN * SUB) * SUB * WIN * 4
    out = pl.pallas_call(
        functools.partial(kernel, chips, cores),
        out_shape=jax.ShapeDtypeStruct((wins, count * rows), jnp.float32),
        in_specs=[hbm, hbm, hbm],
        out_specs=pl.BlockSpec(memory_space=pltpu.VMEM),
        scratch_shapes=scratch + [
            pltpu.SemaphoreType.DMA((3,)),
            pltpu.SemaphoreType.DMA((chips,)),
            pltpu.SemaphoreType.DMA((chips,)),
        ] + [pltpu.SemaphoreType.DMA((count,)) for _ in range(6)],
        compiler_params=pltpu.CompilerParams(
            collective_id=0, has_side_effects=True, vmem_limit_bytes=held + (4 << 20)),
    )(*(pltpu.with_memory_space_constraint(x, pltpu.HBM) for x in (offsets, basis_series, bank)))
    return out.T


def solution(mesh):
    chips, cores = mesh.shape["tmpl"], mesh.shape["det"]
    in_specs = (
        P(None, None, ("groups", "tmpl", "det")),
        P(None, ("groups", "tmpl"), None, None),
        P("groups"),
    )
    out_specs = P(None, ("groups", "tmpl", "det"))
    return jax.shard_map(
        functools.partial(per_device, chips, cores),
        mesh=mesh, in_specs=in_specs, out_specs=out_specs, check_vma=False,
    )
```

```python
import functools
import math

import jax
import jax.numpy as jnp
from jax import lax
from jax.experimental import pallas as pl
from jax.experimental.pallas import tpu as pltpu
from jax.sharding import PartitionSpec as P

WIN = 128
SUB = 8
SLIDE_BLOCKS = 16
SUMS = 16
VMEM_MOST = 62 << 20
MESH = pl.DeviceIdType.MESH
TINY = 1e-18
CODE = jnp.int16
SPAN = 30
STEPS = 1092
TOP = 15


def coded(power):
    log = jnp.log(jnp.maximum(power, 2.0 ** (TOP - 2 * SPAN))) * (STEPS / math.log(2.0))
    return jnp.round(log - (TOP - SPAN) * STEPS).astype(jnp.int32).astype(CODE)


def decoded(code):
    code = code.astype(jnp.int32).astype(jnp.float32)
    power = jnp.exp2(code * (1.0 / STEPS) + (TOP - SPAN))
    return jnp.where(code <= -SPAN * STEPS, 0.0, power)


def kernel(
    chips, cores, adder,
    off_hbm, basis_hbm, bank_hbm, out_ref,
    off_ref, basis_ref, bank_ref, bank_own, bank_all, stage, recv, dec, peaks, final,
    sums, added, part, load, bank_s, fwd_s, pass_s, bank_r, pow_s, pow_r, peak_s, peak_r, sum_s, sum_r,
):
    dets, basis, block = basis_ref.shape
    rows2 = bank_ref.shape[1] // cores
    rows = rows2 // 2
    half = block // 2
    wins = block // WIN
    count = chips * cores
    total = count * wins
    per_row = WIN // rows
    near = chips // 2
    chip, core = lax.axis_index("tmpl"), lax.axis_index("det")
    me = chip * cores + core
    side, place = lax.div(chip, near), lax.rem(chip, near)

    load_bank = pltpu.make_async_copy(bank_hbm, bank_ref, load.at[0])
    load_basis = pltpu.make_async_copy(basis_hbm, basis_ref, load.at[1])
    load_off = pltpu.make_async_copy(off_hbm, off_ref, load.at[2])
    load_bank.start()
    load_basis.start()
    load_off.start()

    def dev(j, c):
        return {"tmpl": j, "det": c}

    def across(j):
        return lax.rem(j + near, chips)

    def close(k):
        if near & (near - 1):
            return side * near + lax.rem(place + near + k, near)
        return side * near + lax.bitwise_xor(place, jnp.int32(k))

    def facing(k):
        return close(-k if near & (near - 1) else k)

    def other_core(d):
        return lax.rem(core + d, cores)

    def over(lo, hi, fn, short=True):
        if short and hi - lo <= 8:
            for k in range(lo, hi):
                fn(k)
            return

        @pl.loop(lo, hi)
        def _(k):
            fn(k)

    def over_peers(fn):
        for d in range(1, cores):
            fn(chip, other_core(d))
        for d in range(cores):
            c = other_core(d)
            over(0, near, lambda k: fn(across(close(k)), c))
            over(1, near, lambda k: fn(close(k), c))

    barrier = pltpu.get_barrier_semaphore()
    over_peers(lambda j, c: pl.semaphore_signal(barrier, inc=1, device_id=dev(j, c), device_id_type=MESH))

    def bank_copy(j, src, sem):
        return pltpu.make_async_remote_copy(
            src_ref=bank_all.at[src], dst_ref=bank_all.at[src], send_sem=sem, recv_sem=bank_r.at[src],
            device_id=dev(j, core), device_id_type=MESH)

    def pass_copy(src, c):
        return pltpu.make_async_remote_copy(
            src_ref=bank_all.at[src], dst_ref=bank_all.at[src],
            send_sem=pass_s.at[lax.div(src, cores) * cores + c], recv_sem=bank_r.at[src],
            device_id=dev(chip, c), device_id_type=MESH)

    def pow_copy(j, c, src):
        return pltpu.make_async_remote_copy(
            src_ref=stage.at[j * cores + c], dst_ref=recv.at[src],
            send_sem=pow_s.at[j * cores + c], recv_sem=pow_r.at[src],
            device_id=dev(j, c), device_id_type=MESH)

    def lift(i):
        return lax.rem(i + near * cores, count)

    def add_copy(j, src):
        slot = across(j) * cores + adder
        return pltpu.make_async_remote_copy(
            src_ref=stage.at[slot], dst_ref=recv.at[lift(src)],
            send_sem=pow_s.at[slot], recv_sem=pow_r.at[lift(src)],
            device_id=dev(j, adder), device_id_type=MESH)

    def sum_copy(q):
        some = pl.ds(q * SUMS, SUMS)
        return pltpu.make_async_remote_copy(
            src_ref=sums.at[some], dst_ref=added.at[some], send_sem=sum_s.at[q], recv_sem=sum_r.at[q],
            device_id=dev(across(chip), adder), device_id_type=MESH)

    def cross(j, fn, own=False):
        if adder is not None:
            add = lambda: fn(add_copy(j, me))
            pl.when(core != adder)(add) if own else add()
        for c in range(cores):
            if c != adder:
                fn(pow_copy(across(j), c, me))

    def peak_row(j, c):
        i = j * cores + c
        return lax.div(i, per_row) * SUB + lax.rem(SUB - lax.rem(i, SUB), SUB)

    def peak_copy(j, c, src):
        return pltpu.make_async_remote_copy(
            src_ref=peaks.at[peak_row(j, c)], dst_ref=final.at[src],
            send_sem=peak_s.at[j * cores + c], recv_sem=peak_r.at[src],
            device_id=dev(j, c), device_id_type=MESH)

    span = dets * rows2
    size = span * cores
    r = lax.broadcasted_iota(jnp.int32, (size, size), 0)
    i = lax.broadcasted_iota(jnp.int32, (size, size), 1)
    c_of = lax.div(r, span)
    d_of = lax.rem(lax.div(r, rows2), dets)
    k_of = lax.rem(lax.div(r, rows), 2)
    m_of = lax.rem(r, rows)
    perm = (i == (d_of * cores + c_of) * rows2 + m_of * 2 + k_of).astype(jnp.float32).astype(jnp.bfloat16)

    def largest(x):
        x = jnp.abs(x).astype(jnp.float32)
        x = jnp.max(x.reshape(-1, SUB, x.shape[-1]), axis=0)
        return jnp.max(jnp.max(x, axis=0, keepdims=True), axis=1, keepdims=True)

    load_bank.wait()
    sorted_bank = jnp.dot(
        perm, bank_ref[...].reshape(size, basis), preferred_element_type=jnp.float32).astype(jnp.bfloat16)
    for c in range(cores):
        bank_own[c, :span] = sorted_bank[c * span:(c + 1) * span]
    load_basis.wait()
    first_rows = lax.broadcasted_iota(jnp.int32, (SUB, basis), 0) < SUB // 2
    top = largest(basis_ref[...].reshape(dets * basis, block))
    for c in range(cores):
        own_max = largest(sorted_bank[c * span:(c + 1) * span])
        note = jnp.where(first_rows, jnp.broadcast_to(top, (SUB, basis)), jnp.broadcast_to(own_max, (SUB, basis)))
        bank_own[c, span:] = note.astype(jnp.bfloat16)
    bank_all[me] = bank_own[core]

    def bank_max(bank, src):
        return bank[src, span:].astype(jnp.float32)[SUB // 2:SUB // 2 + 1, :1]

    def powers_for(j, bank, first):
        to = across(j)
        inv = []
        for c in range(cores):
            a = jnp.maximum(bank_max(bank, first + c) * top, TINY)
            inv.append(1.0 / (a * a))
        for d in range(dets):
            w = jnp.concatenate(
                [bank[first + c, d * rows2:(d + 1) * rows2] for c in range(cores)], axis=0)
            f = jnp.dot(w, basis_ref[d], preferred_element_type=jnp.float32)
            f = f * f
            for c in range(cores):
                p = (f[c * rows2:c * rows2 + rows] + f[c * rows2 + rows:(c + 1) * rows2]) * inv[c]
                stage[to * cores + c, d] = coded(jnp.concatenate([p[:, :half], p[:, half:]], axis=0))

    def pieces(j, fn):
        for d in range(1, cores):
            fn(j * cores + other_core(d))

    powers_for(chip, bank_own, 0)
    if adder is not None:
        @pl.when(core == adder)
        def _():
            dec[...] = jnp.zeros_like(dec)

        @pl.when(core != adder)
        def _():
            part[...] = jnp.zeros_like(part)

    pl.semaphore_wait(barrier, count - 1)

    bank_copy(across(chip), me, bank_s.at[0]).start()
    over(1, near, lambda k: bank_copy(facing(k), me, bank_s.at[k]).start())
    cross(chip, lambda copy: copy.start(), own=True)
    for d in range(1, cores):
        pass_copy(me, other_core(d)).start()

    def pass_on(src):
        bank_copy(chip, src, bank_s.at[0]).wait_recv()
        for d in range(1, cores):
            pass_copy(src, other_core(d)).start()

    over(1, near, lambda k: pass_on(close(k) * cores + core))
    relay = across(chip) * cores + core
    pass_on(relay)
    over(1, near, lambda k: bank_copy(facing(k), relay, fwd_s.at[k]).start())

    def near_powers(k):
        j = close(k)
        pieces(j, lambda src: bank_copy(chip, src, bank_s.at[0]).wait_recv())
        powers_for(j, bank_all, j * cores)
        cross(j, lambda copy: copy.start())

    over(1, near, near_powers, short=False)

    over(1, near, lambda k: pass_on(across(close(k)) * cores + core))
    pieces(across(chip), lambda src: bank_copy(chip, src, bank_s.at[0]).wait_recv())
    powers_for(across(chip), bank_all, across(chip) * cores)
    for d in range(1, cores):
        pow_copy(chip, other_core(d), me).start()

    def far_powers(k):
        j = across(close(k))
        pieces(j, lambda src: bank_copy(chip, src, bank_s.at[0]).wait_recv())
        powers_for(j, bank_all, j * cores)
        for c in range(cores):
            pow_copy(close(k), c, me).start()

    over(1, near, far_powers, short=False)

    load_off.wait()
    rest = [lax.rem(off_ref[d], WIN) for d in range(dets)]
    shifts = [lax.div(off_ref[d], WIN) for d in range(dets)]
    lane = lax.broadcasted_iota(jnp.int32, (rows, WIN), 1)
    inside = [lane < WIN - rest[d] for d in range(dets)]

    def top_of(src):
        return bank_all[src, span:].astype(jnp.float32)[:1, :1]

    def scale_of(top, bank):
        a = jnp.maximum(top * bank, TINY)
        return a * a

    def decode(src, value, bank):
        scale = scale_of(top_of(src), bank)
        for d in range(dets):
            x = decoded(value(d)) * scale
            tiles = []
            for v in range(wins):
                h, q = divmod(v, wins // 2)
                tile = x[h * rows:(h + 1) * rows, q * WIN:(q + 1) * WIN]
                tile = pltpu.roll(tile, WIN - rest[d], 1)
                dec[d, src * wins + v] = tile
                tiles.append(tile)

            @pl.when(src < SLIDE_BLOCKS)
            def _():
                for v in range(wins):
                    dec[d, (count + src) * wins + v] = tiles[v]

    def adding(base):
        last = {}

        def tile(d, v):
            if last.get(d, (None, None))[0] != v:
                last[d] = (v, dec[d, base + shifts[d] + v])
            return last[d][1]

        def leaf(v):
            power = None
            for d in range(dets):
                lo = tile(d, v)
                x = jnp.where(inside[d], lo, tile(d, v + 1))
                power = x if power is None else power + x
            return power

        return leaf

    def far_take():
        @pl.loop(0, near * cores)
        def _(n):
            src = across(close(lax.div(n, cores))) * cores + lax.rem(n, cores)
            pow_copy(chip, core, src).wait_recv()
            decode(src, lambda d: recv[src, d], owned)

    def add_near():
        bank = bank_max(bank_all, me)
        decode(me, lambda d: stage[lift(me), d], bank)

        def take(src):
            pow_copy(chip, core, lift(src)).wait_recv()
            decode(src, lambda d: recv[lift(src), d], bank)

        for d in range(1, cores):
            take(chip * cores + other_core(d))

        @pl.loop(cores, near * cores)
        def _(n):
            take(close(lax.div(n, cores)) * cores + lax.rem(n, cores))

        inv = 1.0 / (4.0 * scale_of(most(lambda k: close(k)), bank))

        @pl.loop(0, total // 2 // SUMS)
        def _(q):
            leaf = adding(q * 2 * SUMS)
            for v in range(SUMS):
                pair = jnp.concatenate([leaf(2 * v), leaf(2 * v + 1)], axis=0)
                sums[q * SUMS + v] = coded(pair * inv)
            sum_copy(q).start()

    def most(chip_of):
        tops = [bank_all[chip_of(k) * cores + c, span:] for k in range(near) for c in range(cores)]
        return functools.reduce(jnp.maximum, [x.astype(jnp.float32) for x in tops])[:1, :1]

    def take_sums():
        scale = 4.0 * scale_of(most(lambda k: across(close(k))), owned)

        @pl.loop(0, total // 2 // SUMS)
        def _(q):
            sum_copy(q).wait_recv()
            for v in range(SUMS):
                x = decoded(added[q * SUMS + v]) * scale
                part[(q * SUMS + v) * 2] = x[:rows]
                part[(q * SUMS + v) * 2 + 1] = x[rows:]

    pieces(chip, lambda src: bank_copy(chip, src, bank_s.at[0]).wait_recv())
    owned = bank_max(bank_all, across(chip) * cores + core)
    if adder is None:
        far_take()
    else:
        pl.when(core == adder)(add_near)
        pl.when(core != adder)(far_take)

    decode(me, lambda d: stage[me, d], owned)

    def take(j, c):
        src = j * cores + c
        pow_copy(chip, core, src).wait_recv()
        decode(src, lambda d: recv[src, d], owned)

    for d in range(1, cores):
        take(chip, other_core(d))

    @pl.loop(cores, near * cores)
    def _(n):
        take(close(lax.div(n, cores)), lax.rem(n, cores))

    if adder is not None:
        pl.when(core == adder)(take_sums)

    bit = [lax.rem(lax.div(lane, 1 << p), 2) == 0 for p in range(7)]
    row = lax.broadcasted_iota(jnp.int32, (rows, WIN), 0)
    dest = lax.rem(SUB - row, SUB) + SUB * lax.div(lane, WIN // 2)
    index = SUB * lax.rem(dest + lax.rem(lane, SUB), per_row) + lax.rem(lax.div(lane, SUB), SUB)

    def group(g):
        base = g * WIN
        near_sum = adding(base)

        def leaf(v):
            return near_sum(v) if adder is None else near_sum(v) + part[base + v]

        def merged(k, v):
            if k == 0:
                return leaf(v)
            p = k - 1
            a = merged(p, v)
            b = merged(p, v + (1 << p))
            s = jnp.where(bit[p], a, b)
            t = jnp.where(bit[p], b, a)
            return jnp.maximum(s, pltpu.roll(t, WIN - (1 << p), 1))

        x = jnp.sqrt(merged(7, 0))
        x = pltpu.roll(x, 0, 1, stride=SUB, stride_axis=0)
        for p in range(3):
            x = jnp.where(bit[3 + p], x, pltpu.roll(x, SUB - (1 << p), 0))
        x = jnp.take_along_axis(x, index, axis=1)
        for s in range(SUB):
            peaks[g * SUB + s] = x[s:s + 1]

    over(0, total // WIN, group, short=total == WIN)

    over_peers(lambda j, c: peak_copy(j, c, me).start())
    final[me] = peaks[peak_row(chip, core)]
    over_peers(lambda j, c: peak_copy(chip, core, j * cores + c).wait_recv())

    high = lax.rem(lax.div(me, SUB), 2) * (WIN // 2)
    e_of = lax.broadcasted_iota(jnp.int32, (per_row, WIN), 0)
    l_of = lax.broadcasted_iota(jnp.int32, (per_row, WIN), 1)
    groups = count // per_row
    for g in range(groups):
        to = (g + groups // 2) % groups if groups > 1 else 0
        x = final[g * per_row:(g + 1) * per_row].reshape(per_row, WIN)
        x = pltpu.roll(x, lax.rem(WIN - high, WIN), 1)
        turn = 0 if groups > 1 else per_row // 2
        x = jnp.concatenate([
            pltpu.roll(x[h:h + SUB], (h + turn) * rows % WIN, 1, stride=rows, stride_axis=0)
            for h in range(0, per_row, SUB)], axis=0)
        for i in range(wins):
            y = pltpu.roll(x, (WIN - i * rows) % WIN, 1)
            y = jnp.where(lax.div(l_of, rows) == lax.rem(e_of + turn, per_row), y, 0.0)
            out_ref[i:i + 1, to * WIN:(to + 1) * WIN] = jnp.sum(y, axis=0, keepdims=True)

    bank_copy(across(chip), me, bank_s.at[0]).wait_send()
    over(1, near, lambda k: bank_copy(facing(k), me, bank_s.at[k]).wait_send())
    over(1, near, lambda k: bank_copy(facing(k), relay, fwd_s.at[k]).wait_send())

    def passed(j):
        for d in range(1, cores):
            pass_copy(j * cores + core, other_core(d)).wait_send()

    over(0, near, lambda k: passed(close(k)))
    over(0, near, lambda k: passed(across(close(k))))

    def drain(k):
        j = close(k)
        for c in range(cores):
            pow_copy(j, c, me).wait_send()

    over(1, near, drain)
    for d in range(1, cores):
        pow_copy(chip, other_core(d), me).wait_send()
    cross(chip, lambda copy: copy.wait_send(), own=True)
    over(1, near, lambda k: cross(close(k), lambda copy: copy.wait_send()))
    over_peers(lambda j, c: peak_copy(j, c, me).wait_send())
    if adder is not None:
        @pl.when(core == adder)
        def _():
            for q in range(total // 2 // SUMS):
                sum_copy(q).wait_send()


def per_device(chips, cores, basis_series, reconstruction, offsets):
    dets, basis, block = basis_series.shape
    templates = reconstruction.shape[1]
    bank = reconstruction.reshape(dets, templates * 2, basis)
    count = chips * cores
    rows = templates // cores
    wins = block // WIN
    total = count * wins
    hbm = pl.BlockSpec(memory_space=pltpu.HBM)
    scratch = [
        pltpu.SMEM(offsets.shape, offsets.dtype),
        pltpu.VMEM(basis_series.shape, basis_series.dtype),
        pltpu.VMEM(bank.shape, bank.dtype),
        pltpu.VMEM((cores, dets * rows * 2 + SUB, basis), jnp.bfloat16),
        pltpu.VMEM((count, dets * rows * 2 + SUB, basis), jnp.bfloat16),
        pltpu.VMEM((count, dets, rows * 2, block // 2), CODE),
        pltpu.VMEM((count, dets, rows * 2, block // 2), CODE),
        pltpu.VMEM((dets, total + SLIDE_BLOCKS * wins, rows, WIN), jnp.float32),
        pltpu.VMEM((total // WIN * SUB, 1, WIN), jnp.float32),
        pltpu.VMEM((count, 1, WIN), jnp.float32),
    ]
    held = sum(math.prod(x.shape) * jnp.dtype(x.dtype).itemsize for x in scratch[1:-2])
    held += (count + total // WIN * SUB) * SUB * WIN * 4 + (4 << 20)
    extra = total * rows * WIN * 8
    adder = cores - 1 if held + extra <= VMEM_MOST and cores > 1 else None
    tiles = total if adder is not None else 2 * SUMS
    scratch += [
        pltpu.VMEM((tiles // 2, rows * 2, WIN), CODE),
        pltpu.VMEM((tiles // 2, rows * 2, WIN), CODE),
        pltpu.VMEM((tiles, rows, WIN), jnp.float32),
    ]
    held += tiles * rows * WIN * 8
    out = pl.pallas_call(
        functools.partial(kernel, chips, cores, adder),
        out_shape=jax.ShapeDtypeStruct((wins, count * rows), jnp.float32),
        in_specs=[hbm, hbm, hbm],
        out_specs=pl.BlockSpec(memory_space=pltpu.VMEM),
        scratch_shapes=scratch + [
            pltpu.SemaphoreType.DMA((3,)),
            pltpu.SemaphoreType.DMA((chips,)),
            pltpu.SemaphoreType.DMA((chips,)),
        ] + [pltpu.SemaphoreType.DMA((count,)) for _ in range(6)]
        + [pltpu.SemaphoreType.DMA((tiles // 2 // SUMS,)) for _ in range(2)],
        compiler_params=pltpu.CompilerParams(
            collective_id=0, has_side_effects=True, vmem_limit_bytes=held),
    )(*(pltpu.with_memory_space_constraint(x, pltpu.HBM) for x in (offsets, basis_series, bank)))
    return out.T


def solution(mesh):
    chips, cores = mesh.shape["tmpl"], mesh.shape["det"]
    in_specs = (
        P(None, None, ("groups", "tmpl", "det")),
        P(None, ("groups", "tmpl"), None, None),
        P("groups"),
    )
    out_specs = P(None, ("groups", "tmpl", "det"))
    return jax.shard_map(
        functools.partial(per_device, chips, cores),
        mesh=mesh, in_specs=in_specs, out_specs=out_specs, check_vma=False,
    )
```

```python
import functools
import math

import jax
import jax.numpy as jnp
from jax import lax
from jax.experimental import pallas as pl
from jax.experimental.pallas import tpu as pltpu
from jax.sharding import PartitionSpec as P

WIN = 128
SUB = 8
SLIDE_BLOCKS = 16
SUMS = 16
VMEM_MOST = 62 << 20
MESH = pl.DeviceIdType.MESH
TINY = 1e-18
CODE = jnp.int16
SPAN = 30
STEPS = 1092
TOP = 15


def coded(power):
    log = jnp.log(jnp.maximum(power, 2.0 ** (TOP - 2 * SPAN))) * (STEPS / math.log(2.0))
    return jnp.round(log - (TOP - SPAN) * STEPS).astype(jnp.int32).astype(CODE)


def decoded(code):
    code = code.astype(jnp.int32).astype(jnp.float32)
    power = jnp.exp2(code * (1.0 / STEPS) + (TOP - SPAN))
    return jnp.where(code <= -SPAN * STEPS, 0.0, power)


def kernel(
    chips, cores, adder,
    off_hbm, basis_hbm, bank_hbm, out_ref,
    off_ref, basis_ref, bank_ref, bank_own, bank_all, stage, recv, dec, peaks, final,
    sums, added, part, load, sent, bank_r, pow_r, peak_r, sum_r,
):
    dets, basis, block = basis_ref.shape
    rows2 = bank_ref.shape[1] // cores
    rows = rows2 // 2
    half = block // 2
    wins = block // WIN
    count = chips * cores
    total = count * wins
    per_row = WIN // rows
    near = chips // 2
    chip, core = lax.axis_index("tmpl"), lax.axis_index("det")
    me = chip * cores + core
    side, place = lax.div(chip, near), lax.rem(chip, near)

    load_bank = pltpu.make_async_copy(bank_hbm, bank_ref, load.at[0])
    load_basis = pltpu.make_async_copy(basis_hbm, basis_ref, load.at[1])
    load_off = pltpu.make_async_copy(off_hbm, off_ref, load.at[2])
    load_bank.start()
    load_basis.start()
    load_off.start()

    def dev(j, c):
        return {"tmpl": j, "det": c}

    def across(j):
        return lax.rem(j + near, chips)

    def close(k):
        return side * near + lax.bitwise_xor(place, jnp.int32(k))

    def other_core(d):
        return lax.rem(core + d, cores)

    def over(lo, hi, fn, short=True):
        if short and hi - lo <= 8:
            for k in range(lo, hi):
                fn(k)
            return

        @pl.loop(lo, hi)
        def _(k):
            fn(k)

    def over_peers(fn):
        for d in range(1, cores):
            fn(chip, other_core(d))
        for d in range(cores):
            c = other_core(d)
            over(0, near, lambda k: fn(across(close(k)), c))
            over(1, near, lambda k: fn(close(k), c))

    barrier = pltpu.get_barrier_semaphore()
    over_peers(lambda j, c: pl.semaphore_signal(barrier, inc=1, device_id=dev(j, c), device_id_type=MESH))

    def bank_copy(j, src):
        return pltpu.make_async_remote_copy(
            src_ref=bank_all.at[src], dst_ref=bank_all.at[src], send_sem=sent.at[0], recv_sem=bank_r.at[src],
            device_id=dev(j, core), device_id_type=MESH)

    def pass_copy(src, c):
        return pltpu.make_async_remote_copy(
            src_ref=bank_all.at[src], dst_ref=bank_all.at[src],
            send_sem=sent.at[0], recv_sem=bank_r.at[src],
            device_id=dev(chip, c), device_id_type=MESH)

    def pow_copy(j, c, src):
        return pltpu.make_async_remote_copy(
            src_ref=stage.at[j * cores + c], dst_ref=recv.at[src],
            send_sem=sent.at[1], recv_sem=pow_r.at[src],
            device_id=dev(j, c), device_id_type=MESH)

    def over_all(ref, sem, n):
        some = ref.at[pl.ds(0, n)]
        return pltpu.make_async_remote_copy(
            src_ref=some, dst_ref=some, send_sem=sem, recv_sem=sem, device_id=dev(chip, core), device_id_type=MESH)

    def lift(i):
        return lax.rem(i + near * cores, count)

    def add_copy(j, src):
        slot = across(j) * cores + adder
        return pltpu.make_async_remote_copy(
            src_ref=stage.at[slot], dst_ref=recv.at[lift(src)],
            send_sem=sent.at[1], recv_sem=pow_r.at[lift(src)],
            device_id=dev(j, adder), device_id_type=MESH)

    def sum_copy(q):
        some = pl.ds(q * SUMS, SUMS)
        return pltpu.make_async_remote_copy(
            src_ref=sums.at[some], dst_ref=added.at[some], send_sem=sent.at[3], recv_sem=sum_r.at[q],
            device_id=dev(across(chip), adder), device_id_type=MESH)

    def near_copy(j, c):
        e = 0 if adder is None else lax.div(c, jnp.int32(adder))
        slot = across(j) * cores + c
        src = lax.rem(me + e * near * cores, count)
        return pltpu.make_async_remote_copy(
            src_ref=stage.at[slot], dst_ref=recv.at[src],
            send_sem=sent.at[1], recv_sem=pow_r.at[src],
            device_id=dev(lax.rem(j + (1 - e) * near, chips), c), device_id_type=MESH)

    def cross(j, fn, own=False):
        if adder is not None:
            add = lambda: fn(add_copy(j, me))
            pl.when(core != adder)(add) if own else add()
        for c in range(cores):
            if c != adder:
                fn(pow_copy(across(j), c, me))

    def peak_row(j, c):
        i = j * cores + c
        return lax.div(i, per_row) * SUB + lax.rem(SUB - lax.rem(i, SUB), SUB)

    def peak_copy(j, c, src):
        return pltpu.make_async_remote_copy(
            src_ref=peaks.at[peak_row(j, c)], dst_ref=final.at[src],
            send_sem=sent.at[2], recv_sem=peak_r.at[0],
            device_id=dev(j, c), device_id_type=MESH)

    span = dets * rows2
    size = span * cores
    r = lax.broadcasted_iota(jnp.int32, (size, size), 0)
    i = lax.broadcasted_iota(jnp.int32, (size, size), 1)
    c_of = lax.div(r, span)
    d_of = lax.rem(lax.div(r, rows2), dets)
    k_of = lax.rem(lax.div(r, rows), 2)
    m_of = lax.rem(r, rows)
    perm = (i == (d_of * cores + c_of) * rows2 + m_of * 2 + k_of).astype(jnp.float32).astype(jnp.bfloat16)

    def largest(x):
        x = jnp.abs(x).astype(jnp.float32)
        x = jnp.max(x.reshape(-1, SUB, x.shape[-1]), axis=0)
        return jnp.max(jnp.max(x, axis=0, keepdims=True), axis=1, keepdims=True)

    load_bank.wait()
    sorted_bank = jnp.dot(
        perm, bank_ref[...].reshape(size, basis), preferred_element_type=jnp.float32).astype(jnp.bfloat16)
    for c in range(cores):
        bank_own[c, :span] = sorted_bank[c * span:(c + 1) * span]
    load_basis.wait()
    first_rows = lax.broadcasted_iota(jnp.int32, (SUB, basis), 0) < SUB // 2
    top = largest(basis_ref[...].reshape(dets * basis, block))
    for c in range(cores):
        own_max = largest(sorted_bank[c * span:(c + 1) * span])
        note = jnp.where(first_rows, jnp.broadcast_to(top, (SUB, basis)), jnp.broadcast_to(own_max, (SUB, basis)))
        bank_own[c, span:] = note.astype(jnp.bfloat16)
    bank_all[me] = bank_own[core]

    def bank_max(bank, src):
        return bank[src, span:].astype(jnp.float32)[SUB // 2:SUB // 2 + 1, :1]

    def powers_for(j, bank, first):
        to = across(j)
        inv = []
        for c in range(cores):
            a = jnp.maximum(bank_max(bank, first + c) * top, TINY)
            inv.append(1.0 / (a * a))
        for d in range(dets):
            w = jnp.concatenate(
                [bank[first + c, d * rows2:(d + 1) * rows2] for c in range(cores)], axis=0)
            f = jnp.dot(w, basis_ref[d], preferred_element_type=jnp.float32)
            f = f * f
            for c in range(cores):
                p = (f[c * rows2:c * rows2 + rows] + f[c * rows2 + rows:(c + 1) * rows2]) * inv[c]
                stage[to * cores + c, d] = coded(jnp.concatenate([p[:, :half], p[:, half:]], axis=0))

    def pieces(j, fn):
        for d in range(1, cores):
            fn(j * cores + other_core(d))

    powers_for(chip, bank_own, 0)
    pl.semaphore_wait(barrier, count - 1)

    bank_copy(across(chip), me).start()
    over(1, near, lambda k: bank_copy(close(k), me).start())
    cross(chip, lambda copy: copy.start(), own=True)
    for d in range(1, cores):
        pass_copy(me, other_core(d)).start()

    if adder is not None:
        @pl.when(core == adder)
        def _():
            dec[...] = jnp.zeros_like(dec)

        @pl.when(core != adder)
        def _():
            part[...] = jnp.zeros_like(part)


    def pass_on(src):
        bank_copy(chip, src).wait_recv()
        for d in range(1, cores):
            pass_copy(src, other_core(d)).start()

    def piece_powers(j, c):
        a = jnp.maximum(bank_max(bank_all, j * cores + c) * top, TINY)
        inv = 1.0 / (a * a)
        for d in range(dets):
            f = jnp.dot(
                bank_all[j * cores + c, d * rows2:(d + 1) * rows2], basis_ref[d], preferred_element_type=jnp.float32)
            f = f * f
            p = (f[:rows] + f[rows:]) * inv
            stage[across(j) * cores + c, d] = coded(jnp.concatenate([p[:, :half], p[:, half:]], axis=0))
        near_copy(j, c).start()

    def near_direct(k):
        pass_on(close(k) * cores + core)
        piece_powers(close(k), core)

    def near_passed(k):
        for d in range(1, cores):
            bank_copy(chip, close(k) * cores + other_core(d)).wait_recv()
            piece_powers(close(k), other_core(d))

    over(1, near // 2, near_direct)
    relay = across(chip) * cores + core
    pass_on(relay)
    over(1, near, lambda k: bank_copy(close(k), relay).start())
    over(near // 2, near, near_direct)
    over(1, near, near_passed, short=False)

    over(1, near, lambda k: pass_on(across(close(k)) * cores + core))
    load_off.wait()
    rest = [lax.rem(off_ref[d], WIN) for d in range(dets)]
    shifts = [lax.div(off_ref[d], WIN) for d in range(dets)]
    lane = lax.broadcasted_iota(jnp.int32, (rows, WIN), 1)
    inside = [lane < WIN - rest[d] for d in range(dets)]

    def top_of(src):
        return bank_all[src, span:].astype(jnp.float32)[:1, :1]

    def scale_of(top, bank):
        a = jnp.maximum(top * bank, TINY)
        return a * a

    def decode(src, value, bank):
        scale = scale_of(top_of(src), bank)
        for d in range(dets):
            x = decoded(value(d)) * scale
            tiles = []
            for v in range(wins):
                h, q = divmod(v, wins // 2)
                tile = x[h * rows:(h + 1) * rows, q * WIN:(q + 1) * WIN]
                tile = pltpu.roll(tile, WIN - rest[d], 1)
                dec[d, src * wins + v] = tile
                tiles.append(tile)

            @pl.when(src < SLIDE_BLOCKS)
            def _():
                for v in range(wins):
                    dec[d, (count + src) * wins + v] = tiles[v]

    def adding(base):
        last = {}

        def tile(d, v):
            if last.get(d, (None, None))[0] != v:
                last[d] = (v, dec[d, base + shifts[d] + v])
            return last[d][1]

        def leaf(v):
            power = None
            for d in range(dets):
                lo = tile(d, v)
                x = jnp.where(inside[d], lo, tile(d, v + 1))
                power = x if power is None else power + x
            return power

        return leaf

    def far_take():
        @pl.loop(0, near * cores)
        def _(n):
            src = across(close(lax.div(n, cores))) * cores + lax.rem(n, cores)
            pow_copy(chip, core, src).wait_recv()
            decode(src, lambda d: recv[src, d], owned)

    def add_near():
        bank = bank_max(bank_all, me)
        decode(me, lambda d: stage[lift(me), d], bank)

        def take(src):
            pow_copy(chip, core, lift(src)).wait_recv()
            decode(src, lambda d: recv[lift(src), d], bank)

        for d in range(1, cores):
            take(chip * cores + other_core(d))

        @pl.loop(cores, near * cores)
        def _(n):
            take(close(lax.div(n, cores)) * cores + lax.rem(n, cores))

        inv = 1.0 / (4.0 * scale_of(most(lambda k: close(k)), bank))

        @pl.loop(0, total // 2 // SUMS)
        def _(q):
            leaf = adding(q * 2 * SUMS)
            for v in range(SUMS):
                pair = jnp.concatenate([leaf(2 * v), leaf(2 * v + 1)], axis=0)
                sums[q * SUMS + v] = coded(pair * inv)
            sum_copy(q).start()

    def most(chip_of):
        tops = [bank_all[chip_of(k) * cores + c, span:] for k in range(near) for c in range(cores)]
        return functools.reduce(jnp.maximum, [x.astype(jnp.float32) for x in tops])[:1, :1]

    def take_sums():
        scale = 4.0 * scale_of(most(lambda k: across(close(k))), owned)

        @pl.loop(0, total // 2 // SUMS)
        def _(q):
            sum_copy(q).wait_recv()
            for v in range(SUMS):
                x = decoded(added[q * SUMS + v]) * scale
                part[(q * SUMS + v) * 2] = x[:rows]
                part[(q * SUMS + v) * 2 + 1] = x[rows:]

    pieces(chip, lambda src: bank_copy(chip, src).wait_recv())
    owned = bank_max(bank_all, across(chip) * cores + core)
    if adder is not None:
        pl.when(core == adder)(add_near)

    pieces(across(chip), lambda src: bank_copy(chip, src).wait_recv())
    powers_for(across(chip), bank_all, across(chip) * cores)
    for d in range(1, cores):
        pow_copy(chip, other_core(d), me).start()

    def far_powers(k):
        j = across(close(k))
        pieces(j, lambda src: bank_copy(chip, src).wait_recv())
        powers_for(j, bank_all, j * cores)
        for c in range(cores):
            pow_copy(close(k), c, me).start()

    over(1, near, far_powers, short=False)

    if adder is None:
        far_take()
    else:
        pl.when(core != adder)(far_take)

    decode(me, lambda d: stage[me, d], owned)

    def take(j, c):
        src = j * cores + c
        pow_copy(chip, core, src).wait_recv()
        decode(src, lambda d: recv[src, d], owned)

    for d in range(1, cores):
        take(chip, other_core(d))

    @pl.loop(cores, near * cores)
    def _(n):
        take(close(lax.div(n, cores)), lax.rem(n, cores))

    if adder is not None:
        pl.when(core == adder)(take_sums)

    bit = [lax.rem(lax.div(lane, 1 << p), 2) == 0 for p in range(7)]
    row = lax.broadcasted_iota(jnp.int32, (rows, WIN), 0)
    dest = lax.rem(SUB - row, SUB) + SUB * lax.div(lane, WIN // 2)
    index = SUB * lax.rem(dest + lax.rem(lane, SUB), per_row) + lax.rem(lax.div(lane, SUB), SUB)

    def group(g):
        base = g * WIN
        near_sum = adding(base)

        def leaf(v):
            return near_sum(v) if adder is None else near_sum(v) + part[base + v]

        def merged(k, v):
            if k == 0:
                return leaf(v)
            p = k - 1
            a = merged(p, v)
            b = merged(p, v + (1 << p))
            s = jnp.where(bit[p], a, b)
            t = jnp.where(bit[p], b, a)
            return jnp.maximum(s, pltpu.roll(t, WIN - (1 << p), 1))

        x = jnp.sqrt(merged(7, 0))
        x = pltpu.roll(x, 0, 1, stride=SUB, stride_axis=0)
        for p in range(3):
            x = jnp.where(bit[3 + p], x, pltpu.roll(x, SUB - (1 << p), 0))
        x = jnp.take_along_axis(x, index, axis=1)
        for s in range(SUB):
            peaks[g * SUB + s] = x[s:s + 1]

    over(0, total // WIN, group, short=total == WIN)

    over_peers(lambda j, c: peak_copy(j, c, me).start())
    final[me] = peaks[peak_row(chip, core)]
    over_all(final, peak_r.at[0], count - 1).wait_recv()

    high = lax.rem(lax.div(me, SUB), 2) * (WIN // 2)
    e_of = lax.broadcasted_iota(jnp.int32, (per_row, WIN), 0)
    l_of = lax.broadcasted_iota(jnp.int32, (per_row, WIN), 1)
    groups = count // per_row
    for g in range(groups):
        to = (g + groups // 2) % groups if groups > 1 else 0
        x = final[g * per_row:(g + 1) * per_row].reshape(per_row, WIN)
        x = pltpu.roll(x, lax.rem(WIN - high, WIN), 1)
        turn = 0 if groups > 1 else per_row // 2
        x = jnp.concatenate([
            pltpu.roll(x[h:h + SUB], (h + turn) * rows % WIN, 1, stride=rows, stride_axis=0)
            for h in range(0, per_row, SUB)], axis=0)
        for i in range(wins):
            y = pltpu.roll(x, (WIN - i * rows) % WIN, 1)
            y = jnp.where(lax.div(l_of, rows) == lax.rem(e_of + turn, per_row), y, 0.0)
            out_ref[i:i + 1, to * WIN:(to + 1) * WIN] = jnp.sum(y, axis=0, keepdims=True)

    banks = near + (near - 1) + chips * (cores - 1)
    over_all(bank_all, sent.at[0], banks).wait_send()
    over_all(final, sent.at[2], count - 1).wait_send()
    if adder is None:
        over_all(stage, sent.at[1], count - 1).wait_send()
    else:
        @pl.when(core == adder)
        def _():
            over_all(stage, sent.at[1], count - 2).wait_send()
            over_all(sums, sent.at[3], total // 2).wait_send()

        @pl.when(core != adder)
        def _():
            over_all(stage, sent.at[1], count - 1).wait_send()


def per_device(chips, cores, basis_series, reconstruction, offsets):
    dets, basis, block = basis_series.shape
    templates = reconstruction.shape[1]
    bank = reconstruction.reshape(dets, templates * 2, basis)
    count = chips * cores
    rows = templates // cores
    wins = block // WIN
    total = count * wins
    hbm = pl.BlockSpec(memory_space=pltpu.HBM)
    scratch = [
        pltpu.SMEM(offsets.shape, offsets.dtype),
        pltpu.VMEM(basis_series.shape, basis_series.dtype),
        pltpu.VMEM(bank.shape, bank.dtype),
        pltpu.VMEM((cores, dets * rows * 2 + SUB, basis), jnp.bfloat16),
        pltpu.VMEM((count, dets * rows * 2 + SUB, basis), jnp.bfloat16),
        pltpu.VMEM((count, dets, rows * 2, block // 2), CODE),
        pltpu.VMEM((count, dets, rows * 2, block // 2), CODE),
        pltpu.VMEM((dets, total + SLIDE_BLOCKS * wins, rows, WIN), jnp.float32),
        pltpu.VMEM((total // WIN * SUB, 1, WIN), jnp.float32),
        pltpu.VMEM((count, 1, WIN), jnp.float32),
    ]
    held = sum(math.prod(x.shape) * jnp.dtype(x.dtype).itemsize for x in scratch[1:-2])
    held += (count + total // WIN * SUB) * SUB * WIN * 4 + (4 << 20)
    extra = total * rows * WIN * 8
    adder = cores - 1 if held + extra <= VMEM_MOST and cores > 1 else None
    tiles = total if adder is not None else 2 * SUMS
    scratch += [
        pltpu.VMEM((tiles // 2, rows * 2, WIN), CODE),
        pltpu.VMEM((tiles // 2, rows * 2, WIN), CODE),
        pltpu.VMEM((tiles, rows, WIN), jnp.float32),
    ]
    held += tiles * rows * WIN * 8
    out = pl.pallas_call(
        functools.partial(kernel, chips, cores, adder),
        out_shape=jax.ShapeDtypeStruct((wins, count * rows), jnp.float32),
        in_specs=[hbm, hbm, hbm],
        out_specs=pl.BlockSpec(memory_space=pltpu.VMEM),
        scratch_shapes=scratch + [
            pltpu.SemaphoreType.DMA((3,)),
            pltpu.SemaphoreType.DMA((4,)),
            pltpu.SemaphoreType.DMA((count,)),
            pltpu.SemaphoreType.DMA((count,)),
            pltpu.SemaphoreType.DMA((1,)),
            pltpu.SemaphoreType.DMA((tiles // 2 // SUMS,)),
        ],
        compiler_params=pltpu.CompilerParams(
            collective_id=0, has_side_effects=True, vmem_limit_bytes=held),
    )(*(pltpu.with_memory_space_constraint(x, pltpu.HBM) for x in (offsets, basis_series, bank)))
    return out.T


def solution(mesh):
    chips, cores = mesh.shape["tmpl"], mesh.shape["det"]
    in_specs = (
        P(None, None, ("groups", "tmpl", "det")),
        P(None, ("groups", "tmpl"), None, None),
        P("groups"),
    )
    out_specs = P(None, ("groups", "tmpl", "det"))
    return jax.shard_map(
        functools.partial(per_device, chips, cores),
        mesh=mesh, in_specs=in_specs, out_specs=out_specs, check_vma=False,
    )
```

```python
import functools
import math

import jax
import jax.numpy as jnp
from jax import lax
from jax.experimental import pallas as pl
from jax.experimental.pallas import tpu as pltpu
from jax.sharding import PartitionSpec as P

WIN = 128
SUB = 8
SLIDE_BLOCKS = 16
SUMS = 16
VMEM_MOST = 62 << 20
MESH = pl.DeviceIdType.MESH
TINY = 1e-18
CODE = jnp.int16
SPAN = 30
STEPS = 1092
TOP = 15


def coded(power):
    log = jnp.log(jnp.maximum(power, 2.0 ** (TOP - 2 * SPAN))) * (STEPS / math.log(2.0))
    return jnp.round(log - (TOP - SPAN) * STEPS).astype(jnp.int32).astype(CODE)


def decoded(code):
    code = code.astype(jnp.int32).astype(jnp.float32)
    power = jnp.exp2(code * (1.0 / STEPS) + (TOP - SPAN))
    return jnp.where(code <= -SPAN * STEPS, 0.0, power)


def kernel(
    chips, cores, adder,
    off_hbm, basis_hbm, bank_hbm, out_ref,
    off_ref, basis_ref, bank_ref, bank_own, bank_all, stage, recv, dec, peaks, final,
    sums, added, part, load, sent, bank_r, pow_r, peak_r, sum_r,
):
    dets, basis, block = basis_ref.shape
    rows2 = bank_ref.shape[1] // cores
    rows = rows2 // 2
    half = block // 2
    wins = block // WIN
    count = chips * cores
    total = count * wins
    per_row = WIN // rows
    near = chips // 2
    chip, core = lax.axis_index("tmpl"), lax.axis_index("det")
    me = chip * cores + core
    side, place = lax.div(chip, near), lax.rem(chip, near)

    load_bank = pltpu.make_async_copy(bank_hbm, bank_ref, load.at[0])
    load_basis = pltpu.make_async_copy(basis_hbm, basis_ref, load.at[1])
    load_off = pltpu.make_async_copy(off_hbm, off_ref, load.at[2])
    load_bank.start()
    load_basis.start()
    load_off.start()

    def dev(j, c):
        return {"tmpl": j, "det": c}

    def across(j):
        return lax.rem(j + near, chips)

    def close(k):
        return side * near + lax.bitwise_xor(place, jnp.int32(k))

    def other_core(d):
        return lax.rem(core + d, cores)

    def over(lo, hi, fn, short=True):
        if short and hi - lo <= 8:
            for k in range(lo, hi):
                fn(k)
            return

        @pl.loop(lo, hi)
        def _(k):
            fn(k)

    def over_peers(fn):
        for d in range(1, cores):
            fn(chip, other_core(d))
        for d in range(cores):
            c = other_core(d)
            over(0, near, lambda k: fn(across(close(k)), c))
            over(1, near, lambda k: fn(close(k), c))

    barrier = pltpu.get_barrier_semaphore()
    over_peers(lambda j, c: pl.semaphore_signal(barrier, inc=1, device_id=dev(j, c), device_id_type=MESH))

    def bank_copy(j, src):
        return pltpu.make_async_remote_copy(
            src_ref=bank_all.at[src], dst_ref=bank_all.at[src], send_sem=sent.at[0], recv_sem=bank_r.at[src],
            device_id=dev(j, core), device_id_type=MESH)

    def pass_copy(src, c):
        return pltpu.make_async_remote_copy(
            src_ref=bank_all.at[src], dst_ref=bank_all.at[src],
            send_sem=sent.at[0], recv_sem=bank_r.at[src],
            device_id=dev(chip, c), device_id_type=MESH)

    def pow_copy(j, c, src):
        return pltpu.make_async_remote_copy(
            src_ref=stage.at[j * cores + c], dst_ref=recv.at[src],
            send_sem=sent.at[1], recv_sem=pow_r.at[src],
            device_id=dev(j, c), device_id_type=MESH)

    def over_all(ref, sem, n):
        some = ref.at[pl.ds(0, n)]
        return pltpu.make_async_remote_copy(
            src_ref=some, dst_ref=some, send_sem=sem, recv_sem=sem, device_id=dev(chip, core), device_id_type=MESH)

    def lift(i):
        return lax.rem(i + near * cores, count)

    def add_copy(j, src):
        slot = across(j) * cores + adder
        return pltpu.make_async_remote_copy(
            src_ref=stage.at[slot], dst_ref=recv.at[lift(src)],
            send_sem=sent.at[1], recv_sem=pow_r.at[lift(src)],
            device_id=dev(j, adder), device_id_type=MESH)

    def sum_copy(q):
        some = pl.ds(q * SUMS, SUMS)
        return pltpu.make_async_remote_copy(
            src_ref=sums.at[some], dst_ref=added.at[some], send_sem=sent.at[3], recv_sem=sum_r.at[q],
            device_id=dev(across(chip), adder), device_id_type=MESH)

    def near_copy(j, c):
        e = 0 if adder is None else lax.div(c, jnp.int32(adder))
        slot = across(j) * cores + c
        src = lax.rem(me + e * near * cores, count)
        return pltpu.make_async_remote_copy(
            src_ref=stage.at[slot], dst_ref=recv.at[src],
            send_sem=sent.at[1], recv_sem=pow_r.at[src],
            device_id=dev(lax.rem(j + (1 - e) * near, chips), c), device_id_type=MESH)

    def cross(j, fn, own=False):
        if adder is not None:
            add = lambda: fn(add_copy(j, me))
            pl.when(core != adder)(add) if own else add()
        for c in range(cores):
            if c != adder:
                fn(pow_copy(across(j), c, me))

    def peak_row(j, c):
        i = j * cores + c
        return lax.div(i, per_row) * SUB + lax.rem(SUB - lax.rem(i, SUB), SUB)

    def peak_copy(j, c, src):
        return pltpu.make_async_remote_copy(
            src_ref=peaks.at[peak_row(j, c)], dst_ref=final.at[src],
            send_sem=sent.at[2], recv_sem=peak_r.at[0],
            device_id=dev(j, c), device_id_type=MESH)

    span = dets * rows2
    size = span * cores
    r = lax.broadcasted_iota(jnp.int32, (size, size), 0)
    i = lax.broadcasted_iota(jnp.int32, (size, size), 1)
    c_of = lax.div(r, span)
    d_of = lax.rem(lax.div(r, rows2), dets)
    k_of = lax.rem(lax.div(r, rows), 2)
    m_of = lax.rem(r, rows)
    perm = (i == (d_of * cores + c_of) * rows2 + m_of * 2 + k_of).astype(jnp.float32).astype(jnp.bfloat16)

    def largest(x):
        x = jnp.abs(x).astype(jnp.float32)
        x = jnp.max(x.reshape(-1, SUB, x.shape[-1]), axis=0)
        return jnp.max(jnp.max(x, axis=0, keepdims=True), axis=1, keepdims=True)

    load_bank.wait()
    sorted_bank = jnp.dot(
        perm, bank_ref[...].reshape(size, basis), preferred_element_type=jnp.float32).astype(jnp.bfloat16)
    for c in range(cores):
        bank_own[c, :span] = sorted_bank[c * span:(c + 1) * span]
    load_basis.wait()
    first_rows = lax.broadcasted_iota(jnp.int32, (SUB, basis), 0) < SUB // 2
    top = largest(basis_ref[...].reshape(dets * basis, block))
    for c in range(cores):
        own_max = largest(sorted_bank[c * span:(c + 1) * span])
        note = jnp.where(first_rows, jnp.broadcast_to(top, (SUB, basis)), jnp.broadcast_to(own_max, (SUB, basis)))
        bank_own[c, span:] = note.astype(jnp.bfloat16)
    bank_all[me] = bank_own[core]

    def bank_max(bank, src):
        return bank[src, span:].astype(jnp.float32)[SUB // 2:SUB // 2 + 1, :1]

    def powers_for(j, bank, first):
        to = across(j)
        inv = []
        for c in range(cores):
            a = jnp.maximum(bank_max(bank, first + c) * top, TINY)
            inv.append(1.0 / (a * a))
        for d in range(dets):
            w = jnp.concatenate(
                [bank[first + c, d * rows2:(d + 1) * rows2] for c in range(cores)], axis=0)
            f = jnp.dot(w, basis_ref[d], preferred_element_type=jnp.float32)
            f = f * f
            for c in range(cores):
                p = (f[c * rows2:c * rows2 + rows] + f[c * rows2 + rows:(c + 1) * rows2]) * inv[c]
                stage[to * cores + c, d] = coded(jnp.concatenate([p[:, :half], p[:, half:]], axis=0))

    def pieces(j, fn):
        for d in range(1, cores):
            fn(j * cores + other_core(d))

    powers_for(chip, bank_own, 0)
    pl.semaphore_wait(barrier, count - 1)

    bank_copy(across(chip), me).start()
    over(1, near, lambda k: bank_copy(close(k), me).start())
    cross(chip, lambda copy: copy.start(), own=True)
    for d in range(1, cores):
        pass_copy(me, other_core(d)).start()

    if adder is not None:
        @pl.when(core == adder)
        def _():
            dec[...] = jnp.zeros_like(dec)

        @pl.when(core != adder)
        def _():
            part[...] = jnp.zeros_like(part)


    def pass_on(src):
        bank_copy(chip, src).wait_recv()
        for d in range(1, cores):
            pass_copy(src, other_core(d)).start()

    def piece_powers(j, c):
        a = jnp.maximum(bank_max(bank_all, j * cores + c) * top, TINY)
        inv = 1.0 / (a * a)
        for d in range(dets):
            f = jnp.dot(
                bank_all[j * cores + c, d * rows2:(d + 1) * rows2], basis_ref[d], preferred_element_type=jnp.float32)
            f = f * f
            p = (f[:rows] + f[rows:]) * inv
            stage[across(j) * cores + c, d] = coded(jnp.concatenate([p[:, :half], p[:, half:]], axis=0))

    def near_direct(k, hold=False):
        pass_on(close(k) * cores + core)
        piece_powers(close(k), core)
        copy = near_copy(close(k), core)
        if not hold or adder is None:
            copy.start()
        else:
            pl.when(core == adder)(copy.start)

    def near_passed(k):
        for d in range(1, cores):
            bank_copy(chip, close(k) * cores + other_core(d)).wait_recv()
            piece_powers(close(k), other_core(d))
            near_copy(close(k), other_core(d)).start()

    near_direct(near // 2)
    relay = across(chip) * cores + core
    pass_on(relay)
    over(1, near, lambda k: bank_copy(close(k), relay).start())
    over(1, near // 2, lambda k: near_direct(near - k, True))
    over(1, near // 2, lambda k: near_direct(near // 2 - k, True))
    over(1, near, near_passed, short=False)

    def release(k):
        if adder is not None:
            pl.when(core != adder)(near_copy(close(k), core).start)

    over(1, near // 2, lambda k: release(near - k))
    over(1, near // 2, lambda k: release(near // 2 - k))

    over(1, near, lambda k: pass_on(across(close(k)) * cores + core))
    load_off.wait()
    rest = [lax.rem(off_ref[d], WIN) for d in range(dets)]
    shifts = [lax.div(off_ref[d], WIN) for d in range(dets)]
    lane = lax.broadcasted_iota(jnp.int32, (rows, WIN), 1)
    inside = [lane < WIN - rest[d] for d in range(dets)]

    def top_of(src):
        return bank_all[src, span:].astype(jnp.float32)[:1, :1]

    def scale_of(top, bank):
        a = jnp.maximum(top * bank, TINY)
        return a * a

    def decode(src, value, bank):
        scale = scale_of(top_of(src), bank)
        for d in range(dets):
            x = decoded(value(d)) * scale
            tiles = []
            for v in range(wins):
                h, q = divmod(v, wins // 2)
                tile = x[h * rows:(h + 1) * rows, q * WIN:(q + 1) * WIN]
                tile = pltpu.roll(tile, WIN - rest[d], 1)
                dec[d, src * wins + v] = tile
                tiles.append(tile)

            @pl.when(src < SLIDE_BLOCKS)
            def _():
                for v in range(wins):
                    dec[d, (count + src) * wins + v] = tiles[v]

    def adding(base):
        last = {}

        def tile(d, v):
            if last.get(d, (None, None))[0] != v:
                last[d] = (v, dec[d, base + shifts[d] + v])
            return last[d][1]

        def leaf(v):
            power = None
            for d in range(dets):
                lo = tile(d, v)
                x = jnp.where(inside[d], lo, tile(d, v + 1))
                power = x if power is None else power + x
            return power

        return leaf

    def far_take():
        @pl.loop(0, near * cores)
        def _(n):
            src = across(close(lax.div(n, cores))) * cores + lax.rem(n, cores)
            pow_copy(chip, core, src).wait_recv()
            decode(src, lambda d: recv[src, d], owned)

    def add_near():
        bank = bank_max(bank_all, me)
        decode(me, lambda d: stage[lift(me), d], bank)

        def take(src):
            pow_copy(chip, core, lift(src)).wait_recv()
            decode(src, lambda d: recv[lift(src), d], bank)

        for d in range(1, cores):
            take(chip * cores + other_core(d))

        @pl.loop(cores, near * cores)
        def _(n):
            take(close(lax.div(n, cores)) * cores + lax.rem(n, cores))

        inv = 1.0 / (4.0 * scale_of(most(lambda k: close(k)), bank))

        @pl.loop(0, total // 2 // SUMS)
        def _(q):
            leaf = adding(q * 2 * SUMS)
            for v in range(SUMS):
                pair = jnp.concatenate([leaf(2 * v), leaf(2 * v + 1)], axis=0)
                sums[q * SUMS + v] = coded(pair * inv)
            sum_copy(q).start()

    def most(chip_of):
        tops = [bank_all[chip_of(k) * cores + c, span:] for k in range(near) for c in range(cores)]
        return functools.reduce(jnp.maximum, [x.astype(jnp.float32) for x in tops])[:1, :1]

    def take_sums():
        scale = 4.0 * scale_of(most(lambda k: across(close(k))), owned)

        @pl.loop(0, total // 2 // SUMS)
        def _(q):
            sum_copy(q).wait_recv()
            for v in range(SUMS):
                x = decoded(added[q * SUMS + v]) * scale
                part[(q * SUMS + v) * 2] = x[:rows]
                part[(q * SUMS + v) * 2 + 1] = x[rows:]

    pieces(chip, lambda src: bank_copy(chip, src).wait_recv())
    owned = bank_max(bank_all, across(chip) * cores + core)
    if adder is not None:
        pl.when(core == adder)(add_near)

    pieces(across(chip), lambda src: bank_copy(chip, src).wait_recv())
    powers_for(across(chip), bank_all, across(chip) * cores)
    for d in range(1, cores):
        pow_copy(chip, other_core(d), me).start()

    def far_powers(k):
        j = across(close(k))
        pieces(j, lambda src: bank_copy(chip, src).wait_recv())
        powers_for(j, bank_all, j * cores)
        for c in range(cores):
            pow_copy(close(k), c, me).start()

    over(1, near, far_powers, short=False)

    if adder is None:
        far_take()
    else:
        pl.when(core != adder)(far_take)

    decode(me, lambda d: stage[me, d], owned)

    def take(j, c):
        src = j * cores + c
        pow_copy(chip, core, src).wait_recv()
        decode(src, lambda d: recv[src, d], owned)

    for d in range(1, cores):
        take(chip, other_core(d))

    @pl.loop(cores, near * cores)
    def _(n):
        take(close(lax.div(n, cores)), lax.rem(n, cores))

    if adder is not None:
        pl.when(core == adder)(take_sums)

    bit = [lax.rem(lax.div(lane, 1 << p), 2) == 0 for p in range(7)]
    row = lax.broadcasted_iota(jnp.int32, (rows, WIN), 0)
    dest = lax.rem(SUB - row, SUB) + SUB * lax.div(lane, WIN // 2)
    index = SUB * lax.rem(dest + lax.rem(lane, SUB), per_row) + lax.rem(lax.div(lane, SUB), SUB)

    def group(g):
        base = g * WIN
        near_sum = adding(base)

        def leaf(v):
            return near_sum(v) if adder is None else near_sum(v) + part[base + v]

        def merged(k, v):
            if k == 0:
                return leaf(v)
            p = k - 1
            a = merged(p, v)
            b = merged(p, v + (1 << p))
            s = jnp.where(bit[p], a, b)
            t = jnp.where(bit[p], b, a)
            return jnp.maximum(s, pltpu.roll(t, WIN - (1 << p), 1))

        x = jnp.sqrt(merged(7, 0))
        x = pltpu.roll(x, 0, 1, stride=SUB, stride_axis=0)
        for p in range(3):
            x = jnp.where(bit[3 + p], x, pltpu.roll(x, SUB - (1 << p), 0))
        x = jnp.take_along_axis(x, index, axis=1)
        for s in range(SUB):
            peaks[g * SUB + s] = x[s:s + 1]

    over(0, total // WIN, group, short=total == WIN)

    over_peers(lambda j, c: peak_copy(j, c, me).start())
    final[me] = peaks[peak_row(chip, core)]
    over_all(final, peak_r.at[0], count - 1).wait_recv()

    high = lax.rem(lax.div(me, SUB), 2) * (WIN // 2)
    e_of = lax.broadcasted_iota(jnp.int32, (per_row, WIN), 0)
    l_of = lax.broadcasted_iota(jnp.int32, (per_row, WIN), 1)
    groups = count // per_row
    for g in range(groups):
        to = (g + groups // 2) % groups if groups > 1 else 0
        x = final[g * per_row:(g + 1) * per_row].reshape(per_row, WIN)
        x = pltpu.roll(x, lax.rem(WIN - high, WIN), 1)
        turn = 0 if groups > 1 else per_row // 2
        x = jnp.concatenate([
            pltpu.roll(x[h:h + SUB], (h + turn) * rows % WIN, 1, stride=rows, stride_axis=0)
            for h in range(0, per_row, SUB)], axis=0)
        for i in range(wins):
            y = pltpu.roll(x, (WIN - i * rows) % WIN, 1)
            y = jnp.where(lax.div(l_of, rows) == lax.rem(e_of + turn, per_row), y, 0.0)
            out_ref[i:i + 1, to * WIN:(to + 1) * WIN] = jnp.sum(y, axis=0, keepdims=True)

    banks = near + (near - 1) + chips * (cores - 1)
    over_all(bank_all, sent.at[0], banks).wait_send()
    over_all(final, sent.at[2], count - 1).wait_send()
    if adder is None:
        over_all(stage, sent.at[1], count - 1).wait_send()
    else:
        @pl.when(core == adder)
        def _():
            over_all(stage, sent.at[1], count - 2).wait_send()
            over_all(sums, sent.at[3], total // 2).wait_send()

        @pl.when(core != adder)
        def _():
            over_all(stage, sent.at[1], count - 1).wait_send()


def per_device(chips, cores, basis_series, reconstruction, offsets):
    dets, basis, block = basis_series.shape
    templates = reconstruction.shape[1]
    bank = reconstruction.reshape(dets, templates * 2, basis)
    count = chips * cores
    rows = templates // cores
    wins = block // WIN
    total = count * wins
    hbm = pl.BlockSpec(memory_space=pltpu.HBM)
    scratch = [
        pltpu.SMEM(offsets.shape, offsets.dtype),
        pltpu.VMEM(basis_series.shape, basis_series.dtype),
        pltpu.VMEM(bank.shape, bank.dtype),
        pltpu.VMEM((cores, dets * rows * 2 + SUB, basis), jnp.bfloat16),
        pltpu.VMEM((count, dets * rows * 2 + SUB, basis), jnp.bfloat16),
        pltpu.VMEM((count, dets, rows * 2, block // 2), CODE),
        pltpu.VMEM((count, dets, rows * 2, block // 2), CODE),
        pltpu.VMEM((dets, total + SLIDE_BLOCKS * wins, rows, WIN), jnp.float32),
        pltpu.VMEM((total // WIN * SUB, 1, WIN), jnp.float32),
        pltpu.VMEM((count, 1, WIN), jnp.float32),
    ]
    held = sum(math.prod(x.shape) * jnp.dtype(x.dtype).itemsize for x in scratch[1:-2])
    held += (count + total // WIN * SUB) * SUB * WIN * 4 + (4 << 20)
    extra = total * rows * WIN * 8
    adder = cores - 1 if held + extra <= VMEM_MOST and cores > 1 else None
    tiles = total if adder is not None else 2 * SUMS
    scratch += [
        pltpu.VMEM((tiles // 2, rows * 2, WIN), CODE),
        pltpu.VMEM((tiles // 2, rows * 2, WIN), CODE),
        pltpu.VMEM((tiles, rows, WIN), jnp.float32),
    ]
    held += tiles * rows * WIN * 8
    out = pl.pallas_call(
        functools.partial(kernel, chips, cores, adder),
        out_shape=jax.ShapeDtypeStruct((wins, count * rows), jnp.float32),
        in_specs=[hbm, hbm, hbm],
        out_specs=pl.BlockSpec(memory_space=pltpu.VMEM),
        scratch_shapes=scratch + [
            pltpu.SemaphoreType.DMA((3,)),
            pltpu.SemaphoreType.DMA((4,)),
            pltpu.SemaphoreType.DMA((count,)),
            pltpu.SemaphoreType.DMA((count,)),
            pltpu.SemaphoreType.DMA((1,)),
            pltpu.SemaphoreType.DMA((tiles // 2 // SUMS,)),
        ],
        compiler_params=pltpu.CompilerParams(
            collective_id=0, has_side_effects=True, vmem_limit_bytes=held),
    )(*(pltpu.with_memory_space_constraint(x, pltpu.HBM) for x in (offsets, basis_series, bank)))
    return out.T


def solution(mesh):
    chips, cores = mesh.shape["tmpl"], mesh.shape["det"]
    in_specs = (
        P(None, None, ("groups", "tmpl", "det")),
        P(None, ("groups", "tmpl"), None, None),
        P("groups"),
    )
    out_specs = P(None, ("groups", "tmpl", "det"))
    return jax.shard_map(
        functools.partial(per_device, chips, cores),
        mesh=mesh, in_specs=in_specs, out_specs=out_specs, check_vma=False,
    )
```

```python
import functools
import math

import jax
import jax.numpy as jnp
from jax import lax
from jax.experimental import pallas as pl
from jax.experimental.pallas import tpu as pltpu
from jax.sharding import PartitionSpec as P

WIN = 128
SUB = 8
SLIDE_BLOCKS = 16
SUMS = 16
VMEM_MOST = 62 << 20
MESH = pl.DeviceIdType.MESH
TINY = 1e-18
CODE = jnp.int16
SPAN = 30
STEPS = 1092
TOP = 15


def coded(power):
    log = jnp.log(jnp.maximum(power, 2.0 ** (TOP - 2 * SPAN))) * (STEPS / math.log(2.0))
    return jnp.round(log - (TOP - SPAN) * STEPS).astype(jnp.int32).astype(CODE)


def decoded(code):
    code = code.astype(jnp.int32).astype(jnp.float32)
    power = jnp.exp2(code * (1.0 / STEPS) + (TOP - SPAN))
    return jnp.where(code <= -SPAN * STEPS, 0.0, power)


def kernel(
    chips, cores, adder,
    off_hbm, basis_hbm, bank_hbm, out_ref,
    off_ref, basis_ref, bank_ref, bank_own, bank_all, stage, recv, dec, peaks, final,
    sums, added, part, load, sent, bank_r, pow_r, peak_r, sum_r,
):
    dets, basis, block = basis_ref.shape
    rows2 = bank_ref.shape[1] // cores
    rows = rows2 // 2
    half = block // 2
    wins = block // WIN
    count = chips * cores
    total = count * wins
    per_row = WIN // rows
    near = chips // 2
    chip, core = lax.axis_index("tmpl"), lax.axis_index("det")
    me = chip * cores + core
    side, place = lax.div(chip, near), lax.rem(chip, near)

    load_bank = pltpu.make_async_copy(bank_hbm, bank_ref, load.at[0])
    load_basis = pltpu.make_async_copy(basis_hbm, basis_ref, load.at[1])
    load_off = pltpu.make_async_copy(off_hbm, off_ref, load.at[2])
    load_bank.start()
    load_basis.start()
    load_off.start()

    def dev(j, c):
        return {"tmpl": j, "det": c}

    def across(j):
        return lax.rem(j + near, chips)

    def close(k):
        return side * near + lax.bitwise_xor(place, jnp.int32(k))

    def other_core(d):
        return lax.rem(core + d, cores)

    def over(lo, hi, fn, short=True):
        if short and hi - lo <= 8:
            for k in range(lo, hi):
                fn(k)
            return

        @pl.loop(lo, hi)
        def _(k):
            fn(k)

    def over_peers(fn):
        for d in range(1, cores):
            fn(chip, other_core(d))
        for d in range(cores):
            c = other_core(d)
            over(0, near, lambda k: fn(across(close(k)), c))
            over(1, near, lambda k: fn(close(k), c))

    barrier = pltpu.get_barrier_semaphore()
    over_peers(lambda j, c: pl.semaphore_signal(barrier, inc=1, device_id=dev(j, c), device_id_type=MESH))

    def bank_copy(j, src):
        return pltpu.make_async_remote_copy(
            src_ref=bank_all.at[src], dst_ref=bank_all.at[src], send_sem=sent.at[0], recv_sem=bank_r.at[src],
            device_id=dev(j, core), device_id_type=MESH)

    def pass_copy(src, c):
        return pltpu.make_async_remote_copy(
            src_ref=bank_all.at[src], dst_ref=bank_all.at[src],
            send_sem=sent.at[0], recv_sem=bank_r.at[src],
            device_id=dev(chip, c), device_id_type=MESH)

    def pow_copy(j, c, src):
        return pltpu.make_async_remote_copy(
            src_ref=stage.at[j * cores + c], dst_ref=recv.at[src],
            send_sem=sent.at[1], recv_sem=pow_r.at[src],
            device_id=dev(j, c), device_id_type=MESH)

    def over_all(ref, sem, n):
        some = ref.at[pl.ds(0, n)]
        return pltpu.make_async_remote_copy(
            src_ref=some, dst_ref=some, send_sem=sem, recv_sem=sem, device_id=dev(chip, core), device_id_type=MESH)

    def lift(i):
        return lax.rem(i + near * cores, count)

    def add_copy(j, src):
        slot = across(j) * cores + adder
        return pltpu.make_async_remote_copy(
            src_ref=stage.at[slot], dst_ref=recv.at[lift(src)],
            send_sem=sent.at[1], recv_sem=pow_r.at[lift(src)],
            device_id=dev(j, adder), device_id_type=MESH)

    def sum_copy(q):
        some = pl.ds(q * SUMS, SUMS)
        return pltpu.make_async_remote_copy(
            src_ref=sums.at[some], dst_ref=added.at[some], send_sem=sent.at[3], recv_sem=sum_r.at[q],
            device_id=dev(across(chip), adder), device_id_type=MESH)

    def near_copy(j, c):
        e = 0 if adder is None else lax.div(c, jnp.int32(adder))
        slot = across(j) * cores + c
        src = lax.rem(me + e * near * cores, count)
        return pltpu.make_async_remote_copy(
            src_ref=stage.at[slot], dst_ref=recv.at[src],
            send_sem=sent.at[1], recv_sem=pow_r.at[src],
            device_id=dev(lax.rem(j + (1 - e) * near, chips), c), device_id_type=MESH)

    def cross(j, fn, own=False):
        if adder is not None:
            add = lambda: fn(add_copy(j, me))
            pl.when(core != adder)(add) if own else add()
        for c in range(cores):
            if c != adder:
                fn(pow_copy(across(j), c, me))

    def peak_row(j, c):
        i = j * cores + c
        return lax.div(i, per_row) * SUB + lax.rem(SUB - lax.rem(i, SUB), SUB)

    def peak_copy(j, c, src):
        return pltpu.make_async_remote_copy(
            src_ref=peaks.at[peak_row(j, c)], dst_ref=final.at[src],
            send_sem=sent.at[2], recv_sem=peak_r.at[0],
            device_id=dev(j, c), device_id_type=MESH)

    span = dets * rows2
    size = span * cores
    r = lax.broadcasted_iota(jnp.int32, (size, size), 0)
    i = lax.broadcasted_iota(jnp.int32, (size, size), 1)
    c_of = lax.div(r, span)
    d_of = lax.rem(lax.div(r, rows2), dets)
    k_of = lax.rem(lax.div(r, rows), 2)
    m_of = lax.rem(r, rows)
    perm = (i == (d_of * cores + c_of) * rows2 + m_of * 2 + k_of).astype(jnp.float32).astype(jnp.bfloat16)

    def largest(x):
        x = jnp.abs(x).astype(jnp.float32)
        x = jnp.max(x.reshape(-1, SUB, x.shape[-1]), axis=0)
        return jnp.max(jnp.max(x, axis=0, keepdims=True), axis=1, keepdims=True)

    load_bank.wait()
    sorted_bank = jnp.dot(
        perm, bank_ref[...].reshape(size, basis), preferred_element_type=jnp.float32).astype(jnp.bfloat16)
    for c in range(cores):
        bank_own[c, :span] = sorted_bank[c * span:(c + 1) * span]
    load_basis.wait()
    first_rows = lax.broadcasted_iota(jnp.int32, (SUB, basis), 0) < SUB // 2
    top = largest(basis_ref[...].reshape(dets * basis, block))
    for c in range(cores):
        own_max = largest(sorted_bank[c * span:(c + 1) * span])
        note = jnp.where(first_rows, jnp.broadcast_to(top, (SUB, basis)), jnp.broadcast_to(own_max, (SUB, basis)))
        bank_own[c, span:] = note.astype(jnp.bfloat16)
    bank_all[me] = bank_own[core]

    def bank_max(bank, src):
        return bank[src, span:].astype(jnp.float32)[SUB // 2:SUB // 2 + 1, :1]

    def powers_for(j, bank, first):
        to = across(j)
        inv = []
        for c in range(cores):
            a = jnp.maximum(bank_max(bank, first + c) * top, TINY)
            inv.append(1.0 / (a * a))
        for d in range(dets):
            w = jnp.concatenate(
                [bank[first + c, d * rows2:(d + 1) * rows2] for c in range(cores)], axis=0)
            f = jnp.dot(w, basis_ref[d], preferred_element_type=jnp.float32)
            f = f * f
            for c in range(cores):
                p = (f[c * rows2:c * rows2 + rows] + f[c * rows2 + rows:(c + 1) * rows2]) * inv[c]
                stage[to * cores + c, d] = coded(jnp.concatenate([p[:, :half], p[:, half:]], axis=0))

    def pieces(j, fn):
        for d in range(1, cores):
            fn(j * cores + other_core(d))

    powers_for(chip, bank_own, 0)
    pl.semaphore_wait(barrier, count - 1)

    bank_copy(across(chip), me).start()
    over(1, near, lambda k: bank_copy(close(k), me).start())
    cross(chip, lambda copy: copy.start(), own=True)
    for d in range(1, cores):
        pass_copy(me, other_core(d)).start()

    def clear_edges():
        @pl.loop(0, count + SLIDE_BLOCKS)
        def _(n):
            for d in range(dets):
                dec[d, n * wins + wins - 1] = jnp.zeros((rows, WIN), jnp.float32)

    clear_edges()
    if adder is not None:
        @pl.when(core == adder)
        def _():
            dec[...] = jnp.zeros_like(dec)

        @pl.when(core != adder)
        def _():
            part[...] = jnp.zeros_like(part)


    def pass_on(src):
        bank_copy(chip, src).wait_recv()
        for d in range(1, cores):
            pass_copy(src, other_core(d)).start()

    def piece_powers(j, c):
        a = jnp.maximum(bank_max(bank_all, j * cores + c) * top, TINY)
        inv = 1.0 / (a * a)
        for d in range(dets):
            f = jnp.dot(
                bank_all[j * cores + c, d * rows2:(d + 1) * rows2], basis_ref[d], preferred_element_type=jnp.float32)
            f = f * f
            p = (f[:rows] + f[rows:]) * inv
            stage[across(j) * cores + c, d] = coded(jnp.concatenate([p[:, :half], p[:, half:]], axis=0))

    def near_direct(k, hold=False):
        pass_on(close(k) * cores + core)
        piece_powers(close(k), core)
        copy = near_copy(close(k), core)
        if not hold or adder is None:
            copy.start()
        else:
            pl.when(core == adder)(copy.start)

    def near_passed(k):
        for d in range(1, cores):
            bank_copy(chip, close(k) * cores + other_core(d)).wait_recv()
            piece_powers(close(k), other_core(d))
            near_copy(close(k), other_core(d)).start()

    near_direct(near // 2)
    relay = across(chip) * cores + core
    pass_on(relay)
    over(1, near, lambda k: bank_copy(close(k), relay).start())
    over(1, near // 2, lambda k: near_direct(near - k, True))
    over(1, near // 2, lambda k: near_direct(near // 2 - k, True))
    over(1, near, near_passed, short=False)

    def release(k):
        if adder is not None:
            pl.when(core != adder)(near_copy(close(k), core).start)

    over(1, near // 2, lambda k: release(near - k))
    over(1, near // 2, lambda k: release(near // 2 - k))

    over(1, near, lambda k: pass_on(across(close(k)) * cores + core))
    load_off.wait()
    rest = [lax.rem(off_ref[d], WIN) for d in range(dets)]
    shifts = [lax.div(off_ref[d], WIN) for d in range(dets)]
    lane = lax.broadcasted_iota(jnp.int32, (rows, WIN), 1)
    inside = [lane < WIN - rest[d] for d in range(dets)]

    def top_of(src):
        return bank_all[src, span:].astype(jnp.float32)[:1, :1]

    def scale_of(top, bank):
        a = jnp.maximum(top * bank, TINY)
        return a * a

    def kept(index, fn):
        fn(index)
        copied = lambda: fn(total + index)
        copied() if count <= SLIDE_BLOCKS else pl.when(index < SLIDE_BLOCKS * wins)(copied)

    def decode(src, value, bank):
        scale = scale_of(top_of(src), bank)
        first = src * wins
        before = lax.rem(first + total - 1, total)
        for d in range(dets):
            x = decoded(value(d)) * scale
            tiles = []
            for v in range(wins):
                h, q = divmod(v, wins // 2)
                tile = x[h * rows:(h + 1) * rows, q * WIN:(q + 1) * WIN]
                tiles.append(pltpu.roll(tile, WIN - rest[d], 1))
            head = jnp.where(inside[d], 0.0, tiles[0])
            tail = jnp.where(inside[d], tiles[-1], 0.0)

            def joined(at):
                for v in range(wins - 1):
                    dec[d, at + v] = jnp.where(inside[d], tiles[v], tiles[v + 1])
                dec[d, at + wins - 1] += tail

            def ahead(at):
                dec[d, at] += head

            kept(first, joined)
            kept(before, ahead)

    def adding(base):
        def leaf(v):
            power = None
            for d in range(dets):
                x = dec[d, base + shifts[d] + v]
                power = x if power is None else power + x
            return power

        return leaf

    def far_take():
        @pl.loop(0, near * cores)
        def _(n):
            src = across(close(lax.div(n, cores))) * cores + lax.rem(n, cores)
            pow_copy(chip, core, src).wait_recv()
            decode(src, lambda d: recv[src, d], owned)

    def add_near():
        bank = bank_max(bank_all, me)
        decode(me, lambda d: stage[lift(me), d], bank)

        def take(src):
            pow_copy(chip, core, lift(src)).wait_recv()
            decode(src, lambda d: recv[lift(src), d], bank)

        for d in range(1, cores):
            take(chip * cores + other_core(d))

        @pl.loop(cores, near * cores)
        def _(n):
            take(close(lax.div(n, cores)) * cores + lax.rem(n, cores))

        inv = 1.0 / (4.0 * scale_of(most(lambda k: close(k)), bank))

        @pl.loop(0, total // 2 // SUMS)
        def _(q):
            leaf = adding(q * 2 * SUMS)
            for v in range(SUMS):
                pair = jnp.concatenate([leaf(2 * v), leaf(2 * v + 1)], axis=0)
                sums[q * SUMS + v] = coded(pair * inv)
            sum_copy(q).start()

        clear_edges()

    def most(chip_of):
        tops = [bank_all[chip_of(k) * cores + c, span:] for k in range(near) for c in range(cores)]
        return functools.reduce(jnp.maximum, [x.astype(jnp.float32) for x in tops])[:1, :1]

    def take_sums():
        scale = 4.0 * scale_of(most(lambda k: across(close(k))), owned)

        @pl.loop(0, total // 2 // SUMS)
        def _(q):
            sum_copy(q).wait_recv()
            for v in range(SUMS):
                x = decoded(added[q * SUMS + v]) * scale
                part[(q * SUMS + v) * 2] = x[:rows]
                part[(q * SUMS + v) * 2 + 1] = x[rows:]

    pieces(chip, lambda src: bank_copy(chip, src).wait_recv())
    owned = bank_max(bank_all, across(chip) * cores + core)
    if adder is not None:
        pl.when(core == adder)(add_near)

    pieces(across(chip), lambda src: bank_copy(chip, src).wait_recv())
    powers_for(across(chip), bank_all, across(chip) * cores)
    for d in range(1, cores):
        pow_copy(chip, other_core(d), me).start()

    def far_powers(k):
        j = across(close(k))
        pieces(j, lambda src: bank_copy(chip, src).wait_recv())
        powers_for(j, bank_all, j * cores)
        for c in range(cores):
            pow_copy(close(k), c, me).start()

    over(1, near, far_powers, short=False)

    if adder is None:
        far_take()
    else:
        pl.when(core != adder)(far_take)

    decode(me, lambda d: stage[me, d], owned)

    def take(j, c):
        src = j * cores + c
        pow_copy(chip, core, src).wait_recv()
        decode(src, lambda d: recv[src, d], owned)

    for d in range(1, cores):
        take(chip, other_core(d))

    @pl.loop(cores, near * cores)
    def _(n):
        take(close(lax.div(n, cores)), lax.rem(n, cores))

    if adder is not None:
        pl.when(core == adder)(take_sums)

    row = lax.broadcasted_iota(jnp.int32, (rows, WIN), 0)
    dest = lax.rem(SUB - row, SUB) + SUB * lax.div(lane, WIN // 2)
    index = SUB * lax.rem(dest + lax.rem(lane, SUB), per_row) + lax.rem(lax.div(lane, SUB), SUB)

    def group(g):
        base = g * WIN
        near_sum = adding(base)

        def leaf(v):
            return near_sum(v) if adder is None else near_sum(v) + part[base + v]

        x = jnp.zeros((rows, WIN), jnp.float32)
        for v in range(WIN):
            x = jnp.where(lane == v, jnp.max(leaf(v), axis=1, keepdims=True), x)
        x = jnp.sqrt(x)
        x = pltpu.roll(x, 0, 1, stride=SUB, stride_axis=0)
        for p in range(3):
            stay = lax.rem(lax.div(lane, SUB << p), 2) == 0
            x = jnp.where(stay, x, pltpu.roll(x, SUB - (1 << p), 0))
        x = jnp.take_along_axis(x, index, axis=1)
        for s in range(SUB):
            peaks[g * SUB + s] = x[s:s + 1]

    over(0, total // WIN, group, short=total == WIN)

    over_peers(lambda j, c: peak_copy(j, c, me).start())
    final[me] = peaks[peak_row(chip, core)]
    over_all(final, peak_r.at[0], count - 1).wait_recv()

    high = lax.rem(lax.div(me, SUB), 2) * (WIN // 2)
    e_of = lax.broadcasted_iota(jnp.int32, (per_row, WIN), 0)
    l_of = lax.broadcasted_iota(jnp.int32, (per_row, WIN), 1)
    groups = count // per_row
    for g in range(groups):
        to = (g + groups // 2) % groups if groups > 1 else 0
        x = final[g * per_row:(g + 1) * per_row].reshape(per_row, WIN)
        x = pltpu.roll(x, lax.rem(WIN - high, WIN), 1)
        turn = 0 if groups > 1 else per_row // 2
        x = jnp.concatenate([
            pltpu.roll(x[h:h + SUB], (h + turn) * rows % WIN, 1, stride=rows, stride_axis=0)
            for h in range(0, per_row, SUB)], axis=0)
        for i in range(wins):
            y = pltpu.roll(x, (WIN - i * rows) % WIN, 1)
            y = jnp.where(lax.div(l_of, rows) == lax.rem(e_of + turn, per_row), y, 0.0)
            out_ref[i:i + 1, to * WIN:(to + 1) * WIN] = jnp.sum(y, axis=0, keepdims=True)

    banks = near + (near - 1) + chips * (cores - 1)
    over_all(bank_all, sent.at[0], banks).wait_send()
    over_all(final, sent.at[2], count - 1).wait_send()
    if adder is None:
        over_all(stage, sent.at[1], count - 1).wait_send()
    else:
        @pl.when(core == adder)
        def _():
            over_all(stage, sent.at[1], count - 2).wait_send()
            over_all(sums, sent.at[3], total // 2).wait_send()

        @pl.when(core != adder)
        def _():
            over_all(stage, sent.at[1], count - 1).wait_send()


def per_device(chips, cores, basis_series, reconstruction, offsets):
    dets, basis, block = basis_series.shape
    templates = reconstruction.shape[1]
    bank = reconstruction.reshape(dets, templates * 2, basis)
    count = chips * cores
    rows = templates // cores
    wins = block // WIN
    total = count * wins
    hbm = pl.BlockSpec(memory_space=pltpu.HBM)
    scratch = [
        pltpu.SMEM(offsets.shape, offsets.dtype),
        pltpu.VMEM(basis_series.shape, basis_series.dtype),
        pltpu.VMEM(bank.shape, bank.dtype),
        pltpu.VMEM((cores, dets * rows * 2 + SUB, basis), jnp.bfloat16),
        pltpu.VMEM((count, dets * rows * 2 + SUB, basis), jnp.bfloat16),
        pltpu.VMEM((count, dets, rows * 2, block // 2), CODE),
        pltpu.VMEM((count, dets, rows * 2, block // 2), CODE),
        pltpu.VMEM((dets, total + SLIDE_BLOCKS * wins, rows, WIN), jnp.float32),
        pltpu.VMEM((total // WIN * SUB, 1, WIN), jnp.float32),
        pltpu.VMEM((count, 1, WIN), jnp.float32),
    ]
    held = sum(math.prod(x.shape) * jnp.dtype(x.dtype).itemsize for x in scratch[1:-2])
    held += (count + total // WIN * SUB) * SUB * WIN * 4 + (4 << 20)
    extra = total * rows * WIN * 8
    adder = cores - 1 if held + extra <= VMEM_MOST and cores > 1 else None
    tiles = total if adder is not None else 2 * SUMS
    scratch += [
        pltpu.VMEM((tiles // 2, rows * 2, WIN), CODE),
        pltpu.VMEM((tiles // 2, rows * 2, WIN), CODE),
        pltpu.VMEM((tiles, rows, WIN), jnp.float32),
    ]
    held += tiles * rows * WIN * 8
    out = pl.pallas_call(
        functools.partial(kernel, chips, cores, adder),
        out_shape=jax.ShapeDtypeStruct((wins, count * rows), jnp.float32),
        in_specs=[hbm, hbm, hbm],
        out_specs=pl.BlockSpec(memory_space=pltpu.VMEM),
        scratch_shapes=scratch + [
            pltpu.SemaphoreType.DMA((3,)),
            pltpu.SemaphoreType.DMA((4,)),
            pltpu.SemaphoreType.DMA((count,)),
            pltpu.SemaphoreType.DMA((count,)),
            pltpu.SemaphoreType.DMA((1,)),
            pltpu.SemaphoreType.DMA((tiles // 2 // SUMS,)),
        ],
        compiler_params=pltpu.CompilerParams(
            collective_id=0, has_side_effects=True, vmem_limit_bytes=held),
    )(*(pltpu.with_memory_space_constraint(x, pltpu.HBM) for x in (offsets, basis_series, bank)))
    return out.T


def solution(mesh):
    chips, cores = mesh.shape["tmpl"], mesh.shape["det"]
    in_specs = (
        P(None, None, ("groups", "tmpl", "det")),
        P(None, ("groups", "tmpl"), None, None),
        P("groups"),
    )
    out_specs = P(None, ("groups", "tmpl", "det"))
    return jax.shard_map(
        functools.partial(per_device, chips, cores),
        mesh=mesh, in_specs=in_specs, out_specs=out_specs, check_vma=False,
    )
```

```python
import functools
import math

import jax
import jax.numpy as jnp
from jax import lax
from jax.experimental import pallas as pl
from jax.experimental.pallas import tpu as pltpu
from jax.sharding import PartitionSpec as P

WIN = 128
SUB = 8
SLIDE_BLOCKS = 16
SUMS = 32
VMEM_MOST = 62 << 20
MESH = pl.DeviceIdType.MESH
TINY = 1e-18
CODE = jnp.int16
SPAN = 30
STEPS = 1092
TOP = 15


def coded(power):
    log = jnp.log(jnp.maximum(power, 2.0 ** (TOP - 2 * SPAN))) * (STEPS / math.log(2.0))
    return jnp.round(log - (TOP - SPAN) * STEPS).astype(jnp.int32).astype(CODE)


def decoded(code):
    code = code.astype(jnp.int32).astype(jnp.float32)
    power = jnp.exp2(code * (1.0 / STEPS) + (TOP - SPAN))
    return jnp.where(code <= -SPAN * STEPS, 0.0, power)


def kernel(
    chips, cores, adder,
    off_hbm, basis_hbm, bank_hbm, out_ref,
    off_ref, basis_ref, bank_ref, bank_own, bank_all, stage, recv, dec, peaks, final,
    sums, added, part, load, sent, bank_r, pow_r, peak_r, sum_r,
):
    dets, basis, block = basis_ref.shape
    rows2 = bank_ref.shape[1] // cores
    rows = rows2 // 2
    half = block // 2
    wins = block // WIN
    count = chips * cores
    total = count * wins
    per_row = WIN // rows
    near = chips // 2
    chip, core = lax.axis_index("tmpl"), lax.axis_index("det")
    me = chip * cores + core
    side, place = lax.div(chip, near), lax.rem(chip, near)

    load_bank = pltpu.make_async_copy(bank_hbm, bank_ref, load.at[0])
    load_basis = pltpu.make_async_copy(basis_hbm, basis_ref, load.at[1])
    load_off = pltpu.make_async_copy(off_hbm, off_ref, load.at[2])
    load_bank.start()
    load_basis.start()
    load_off.start()

    def dev(j, c):
        return {"tmpl": j, "det": c}

    def across(j):
        return lax.rem(j + near, chips)

    def close(k):
        return side * near + lax.bitwise_xor(place, jnp.int32(k))

    def other_core(d):
        return lax.rem(core + d, cores)

    def over(lo, hi, fn, short=True):
        if short and hi - lo <= 8:
            for k in range(lo, hi):
                fn(k)
            return

        @pl.loop(lo, hi)
        def _(k):
            fn(k)

    def over_peers(fn):
        for d in range(cores):
            over(0, near, lambda k: fn(across(close(k)), other_core(d)))
        for d in range(cores):
            over(1, near, lambda k: fn(close(k), other_core(d)))
        for d in range(1, cores):
            fn(chip, other_core(d))

    barrier = pltpu.get_barrier_semaphore()
    over_peers(lambda j, c: pl.semaphore_signal(barrier, inc=1, device_id=dev(j, c), device_id_type=MESH))

    def bank_copy(j, src):
        return pltpu.make_async_remote_copy(
            src_ref=bank_all.at[src], dst_ref=bank_all.at[src], send_sem=sent.at[0], recv_sem=bank_r.at[src],
            device_id=dev(j, core), device_id_type=MESH)

    def pass_copy(src, c):
        return pltpu.make_async_remote_copy(
            src_ref=bank_all.at[src], dst_ref=bank_all.at[src],
            send_sem=sent.at[0], recv_sem=bank_r.at[src],
            device_id=dev(chip, c), device_id_type=MESH)

    def pow_copy(j, c, src):
        return pltpu.make_async_remote_copy(
            src_ref=stage.at[j * cores + c], dst_ref=recv.at[src],
            send_sem=sent.at[1], recv_sem=pow_r.at[src],
            device_id=dev(j, c), device_id_type=MESH)

    def over_all(ref, sem, n):
        some = ref.at[pl.ds(0, n)]
        return pltpu.make_async_remote_copy(
            src_ref=some, dst_ref=some, send_sem=sem, recv_sem=sem, device_id=dev(chip, core), device_id_type=MESH)

    def lift(i):
        return lax.rem(i + near * cores, count)

    def add_copy(j, src):
        slot = across(j) * cores + adder
        return pltpu.make_async_remote_copy(
            src_ref=stage.at[slot], dst_ref=recv.at[lift(src)],
            send_sem=sent.at[1], recv_sem=pow_r.at[lift(src)],
            device_id=dev(j, adder), device_id_type=MESH)

    def sum_copy(q):
        some = pl.ds(q * SUMS, SUMS)
        return pltpu.make_async_remote_copy(
            src_ref=sums.at[some], dst_ref=added.at[some], send_sem=sent.at[3], recv_sem=sum_r.at[q],
            device_id=dev(across(chip), adder), device_id_type=MESH)

    def near_copy(j, c):
        e = 0 if adder is None else lax.div(c, jnp.int32(adder))
        slot = across(j) * cores + c
        src = lax.rem(me + e * near * cores, count)
        return pltpu.make_async_remote_copy(
            src_ref=stage.at[slot], dst_ref=recv.at[src],
            send_sem=sent.at[1], recv_sem=pow_r.at[src],
            device_id=dev(lax.rem(j + (1 - e) * near, chips), c), device_id_type=MESH)

    def cross(j, fn, own=False):
        if adder is not None:
            add = lambda: fn(add_copy(j, me))
            pl.when(core != adder)(add) if own else add()
        for c in range(cores):
            if c != adder:
                fn(pow_copy(across(j), c, me))

    def peak_row(j, c):
        i = j * cores + c
        return lax.div(i, per_row) * SUB + lax.rem(SUB - lax.rem(i, SUB), SUB)

    def peak_copy(j, c, src):
        return pltpu.make_async_remote_copy(
            src_ref=peaks.at[peak_row(j, c)], dst_ref=final.at[src],
            send_sem=sent.at[2], recv_sem=peak_r.at[0],
            device_id=dev(j, c), device_id_type=MESH)

    span = dets * rows2
    size = span * cores
    r = lax.broadcasted_iota(jnp.int32, (size, size), 0)
    i = lax.broadcasted_iota(jnp.int32, (size, size), 1)
    c_of = lax.div(r, span)
    d_of = lax.rem(lax.div(r, rows2), dets)
    k_of = lax.rem(lax.div(r, rows), 2)
    m_of = lax.rem(r, rows)
    perm = (i == (d_of * cores + c_of) * rows2 + m_of * 2 + k_of).astype(jnp.float32).astype(jnp.bfloat16)

    def largest(x):
        x = jnp.abs(x).astype(jnp.float32)
        x = jnp.max(x.reshape(-1, SUB, x.shape[-1]), axis=0)
        return jnp.max(jnp.max(x, axis=0, keepdims=True), axis=1, keepdims=True)

    load_bank.wait()
    sorted_bank = jnp.dot(
        perm, bank_ref[...].reshape(size, basis), preferred_element_type=jnp.float32).astype(jnp.bfloat16)
    for c in range(cores):
        bank_own[c, :span] = sorted_bank[c * span:(c + 1) * span]
    load_basis.wait()
    first_rows = lax.broadcasted_iota(jnp.int32, (SUB, basis), 0) < SUB // 2
    top = largest(basis_ref[...].reshape(dets * basis, block))
    for c in range(cores):
        own_max = largest(sorted_bank[c * span:(c + 1) * span])
        note = jnp.where(first_rows, jnp.broadcast_to(top, (SUB, basis)), jnp.broadcast_to(own_max, (SUB, basis)))
        bank_own[c, span:] = note.astype(jnp.bfloat16)
    bank_all[me] = bank_own[core]

    def bank_max(bank, src):
        return bank[src, span:].astype(jnp.float32)[SUB // 2:SUB // 2 + 1, :1]

    def powers_for(j, bank, first):
        to = across(j)
        inv = []
        for c in range(cores):
            a = jnp.maximum(bank_max(bank, first + c) * top, TINY)
            inv.append(1.0 / (a * a))
        for d in range(dets):
            w = jnp.concatenate(
                [bank[first + c, d * rows2:(d + 1) * rows2] for c in range(cores)], axis=0)
            f = jnp.dot(w, basis_ref[d], preferred_element_type=jnp.float32)
            f = f * f
            for c in range(cores):
                p = (f[c * rows2:c * rows2 + rows] + f[c * rows2 + rows:(c + 1) * rows2]) * inv[c]
                stage[to * cores + c, d] = coded(jnp.concatenate([p[:, :half], p[:, half:]], axis=0))

    def pieces(j, fn):
        for d in range(1, cores):
            fn(j * cores + other_core(d))

    powers_for(chip, bank_own, 0)
    pl.semaphore_wait(barrier, count - 1)

    bank_copy(across(chip), me).start()
    over(1, near, lambda k: bank_copy(close(k), me).start())
    cross(chip, lambda copy: copy.start(), own=True)
    for d in range(1, cores):
        pass_copy(me, other_core(d)).start()

    def clear_edges():
        @pl.loop(0, count + SLIDE_BLOCKS)
        def _(n):
            for d in range(dets):
                dec[d, n * wins + wins - 1] = jnp.zeros((rows, WIN), jnp.float32)

    clear_edges()
    if adder is not None:
        @pl.when(core == adder)
        def _():
            dec[...] = jnp.zeros_like(dec)

        @pl.when(core != adder)
        def _():
            part[...] = jnp.zeros_like(part)


    def pass_on(src):
        bank_copy(chip, src).wait_recv()
        for d in range(1, cores):
            pass_copy(src, other_core(d)).start()

    def piece_powers(j, c):
        a = jnp.maximum(bank_max(bank_all, j * cores + c) * top, TINY)
        inv = 1.0 / (a * a)
        for d in range(dets):
            f = jnp.dot(
                bank_all[j * cores + c, d * rows2:(d + 1) * rows2], basis_ref[d], preferred_element_type=jnp.float32)
            f = f * f
            p = (f[:rows] + f[rows:]) * inv
            stage[across(j) * cores + c, d] = coded(jnp.concatenate([p[:, :half], p[:, half:]], axis=0))

    def near_direct(k, hold=False):
        pass_on(close(k) * cores + core)
        piece_powers(close(k), core)
        copy = near_copy(close(k), core)
        if not hold or adder is None:
            copy.start()
        else:
            pl.when(core == adder)(copy.start)

    def near_passed(k):
        for d in range(1, cores):
            bank_copy(chip, close(k) * cores + other_core(d)).wait_recv()
            piece_powers(close(k), other_core(d))
            near_copy(close(k), other_core(d)).start()

    near_direct(near // 2)
    relay = across(chip) * cores + core
    pass_on(relay)
    over(1, near, lambda k: bank_copy(close(k), relay).start())
    over(1, near // 2, lambda k: near_direct(near - k, True))
    over(1, near // 2, lambda k: near_direct(near // 2 - k, True))
    over(1, near, near_passed, short=False)

    def release(k):
        if adder is not None:
            pl.when(core != adder)(near_copy(close(k), core).start)

    over(1, near // 2, lambda k: release(near - k))
    over(1, near // 2, lambda k: release(near // 2 - k))

    over(1, near, lambda k: pass_on(across(close(k)) * cores + core))
    load_off.wait()
    rest = [lax.rem(off_ref[d], WIN) for d in range(dets)]
    shifts = [lax.div(off_ref[d], WIN) for d in range(dets)]
    lane = lax.broadcasted_iota(jnp.int32, (rows, WIN), 1)
    inside = [lane < WIN - rest[d] for d in range(dets)]

    def top_of(src):
        return bank_all[src, span:].astype(jnp.float32)[:1, :1]

    def scale_of(top, bank):
        a = jnp.maximum(top * bank, TINY)
        return a * a

    def kept(index, fn):
        fn(index)
        copied = lambda: fn(total + index)
        copied() if count <= SLIDE_BLOCKS else pl.when(index < SLIDE_BLOCKS * wins)(copied)

    def decode(src, value, bank):
        scale = scale_of(top_of(src), bank)
        first = src * wins
        before = lax.rem(first + total - 1, total)
        for d in range(dets):
            x = decoded(value(d)) * scale
            tiles = []
            for v in range(wins):
                h, q = divmod(v, wins // 2)
                tile = x[h * rows:(h + 1) * rows, q * WIN:(q + 1) * WIN]
                tiles.append(pltpu.roll(tile, WIN - rest[d], 1))
            head = jnp.where(inside[d], 0.0, tiles[0])
            tail = jnp.where(inside[d], tiles[-1], 0.0)

            def joined(at):
                for v in range(wins - 1):
                    dec[d, at + v] = jnp.where(inside[d], tiles[v], tiles[v + 1])
                dec[d, at + wins - 1] += tail

            def ahead(at):
                dec[d, at] += head

            kept(first, joined)
            kept(before, ahead)

    def adding(base):
        def leaf(v):
            power = None
            for d in range(dets):
                x = dec[d, base + shifts[d] + v]
                power = x if power is None else power + x
            return power

        return leaf

    def far_take():
        @pl.loop(0, near * cores)
        def _(n):
            src = across(close(lax.div(n, cores))) * cores + lax.rem(n, cores)
            pow_copy(chip, core, src).wait_recv()
            decode(src, lambda d: recv[src, d], owned)

    def add_near():
        bank = bank_max(bank_all, me)
        decode(me, lambda d: stage[lift(me), d], bank)

        def take(src):
            pow_copy(chip, core, lift(src)).wait_recv()
            decode(src, lambda d: recv[lift(src), d], bank)

        for d in range(1, cores):
            take(chip * cores + other_core(d))

        @pl.loop(cores, near * cores)
        def _(n):
            take(close(lax.div(n, cores)) * cores + lax.rem(n, cores))

        inv = 1.0 / (4.0 * scale_of(most(lambda k: close(k)), bank))

        @pl.loop(0, total // 2 // SUMS)
        def _(q):
            leaf = adding(q * 2 * SUMS)
            for v in range(SUMS):
                pair = jnp.concatenate([leaf(2 * v), leaf(2 * v + 1)], axis=0)
                sums[q * SUMS + v] = coded(pair * inv)
            sum_copy(q).start()

        clear_edges()

    def most(chip_of):
        tops = [bank_all[chip_of(k) * cores + c, span:] for k in range(near) for c in range(cores)]
        return functools.reduce(jnp.maximum, [x.astype(jnp.float32) for x in tops])[:1, :1]

    def take_sums():
        scale = 4.0 * scale_of(most(lambda k: across(close(k))), owned)

        @pl.loop(0, total // 2 // SUMS)
        def _(q):
            sum_copy(q).wait_recv()
            for v in range(SUMS):
                x = decoded(added[q * SUMS + v]) * scale
                part[(q * SUMS + v) * 2] = x[:rows]
                part[(q * SUMS + v) * 2 + 1] = x[rows:]

    pieces(chip, lambda src: bank_copy(chip, src).wait_recv())
    owned = bank_max(bank_all, across(chip) * cores + core)
    if adder is not None:
        pl.when(core == adder)(add_near)

    pieces(across(chip), lambda src: bank_copy(chip, src).wait_recv())
    powers_for(across(chip), bank_all, across(chip) * cores)
    for d in range(1, cores):
        pow_copy(chip, other_core(d), me).start()

    def far_powers(k):
        j = across(close(k))
        pieces(j, lambda src: bank_copy(chip, src).wait_recv())
        powers_for(j, bank_all, j * cores)
        for c in range(cores):
            pow_copy(close(k), c, me).start()

    over(1, near, lambda k: far_powers(near - k), short=False)

    if adder is None:
        far_take()
    else:
        pl.when(core != adder)(far_take)

    decode(me, lambda d: stage[me, d], owned)

    def take(j, c):
        src = j * cores + c
        pow_copy(chip, core, src).wait_recv()
        decode(src, lambda d: recv[src, d], owned)

    for d in range(1, cores):
        take(chip, other_core(d))

    @pl.loop(cores, near * cores)
    def _(n):
        take(close(lax.div(n, cores)), lax.rem(n, cores))

    if adder is not None:
        pl.when(core == adder)(take_sums)

    row = lax.broadcasted_iota(jnp.int32, (rows, WIN), 0)
    dest = lax.rem(SUB - row, SUB) + SUB * lax.div(lane, WIN // 2)
    index = SUB * lax.rem(dest + lax.rem(lane, SUB), per_row) + lax.rem(lax.div(lane, SUB), SUB)

    def group(g):
        base = g * WIN
        near_sum = adding(base)

        def leaf(v):
            return near_sum(v) if adder is None else near_sum(v) + part[base + v]

        x = jnp.zeros((rows, WIN), jnp.float32)
        for v in range(WIN):
            x = jnp.where(lane == v, jnp.max(leaf(v), axis=1, keepdims=True), x)
        x = jnp.sqrt(x)
        x = pltpu.roll(x, 0, 1, stride=SUB, stride_axis=0)
        for p in range(3):
            stay = lax.rem(lax.div(lane, SUB << p), 2) == 0
            x = jnp.where(stay, x, pltpu.roll(x, SUB - (1 << p), 0))
        x = jnp.take_along_axis(x, index, axis=1)
        for s in range(SUB):
            peaks[g * SUB + s] = x[s:s + 1]

    over(0, total // WIN, group, short=total == WIN)

    over_peers(lambda j, c: peak_copy(j, c, me).start())
    final[me] = peaks[peak_row(chip, core)]
    banks = near + (near - 1) + chips * (cores - 1)
    over_all(bank_all, sent.at[0], banks).wait_send()
    if adder is None:
        over_all(stage, sent.at[1], count - 1).wait_send()
    else:
        @pl.when(core == adder)
        def _():
            over_all(stage, sent.at[1], count - 2).wait_send()
            over_all(sums, sent.at[3], total // 2).wait_send()

        @pl.when(core != adder)
        def _():
            over_all(stage, sent.at[1], count - 1).wait_send()

    over_all(final, peak_r.at[0], count - 1).wait_recv()

    high = lax.rem(lax.div(me, SUB), 2) * (WIN // 2)
    e_of = lax.broadcasted_iota(jnp.int32, (per_row, WIN), 0)
    l_of = lax.broadcasted_iota(jnp.int32, (per_row, WIN), 1)
    groups = count // per_row
    for g in range(groups):
        to = (g + groups // 2) % groups if groups > 1 else 0
        x = final[g * per_row:(g + 1) * per_row].reshape(per_row, WIN)
        x = pltpu.roll(x, lax.rem(WIN - high, WIN), 1)
        turn = 0 if groups > 1 else per_row // 2
        x = jnp.concatenate([
            pltpu.roll(x[h:h + SUB], (h + turn) * rows % WIN, 1, stride=rows, stride_axis=0)
            for h in range(0, per_row, SUB)], axis=0)
        for i in range(wins):
            y = pltpu.roll(x, (WIN - i * rows) % WIN, 1)
            y = jnp.where(lax.div(l_of, rows) == lax.rem(e_of + turn, per_row), y, 0.0)
            out_ref[i:i + 1, to * WIN:(to + 1) * WIN] = jnp.sum(y, axis=0, keepdims=True)

    over_all(final, sent.at[2], count - 1).wait_send()


def per_device(chips, cores, basis_series, reconstruction, offsets):
    dets, basis, block = basis_series.shape
    templates = reconstruction.shape[1]
    bank = reconstruction.reshape(dets, templates * 2, basis)
    count = chips * cores
    rows = templates // cores
    wins = block // WIN
    total = count * wins
    hbm = pl.BlockSpec(memory_space=pltpu.HBM)
    scratch = [
        pltpu.SMEM(offsets.shape, offsets.dtype),
        pltpu.VMEM(basis_series.shape, basis_series.dtype),
        pltpu.VMEM(bank.shape, bank.dtype),
        pltpu.VMEM((cores, dets * rows * 2 + SUB, basis), jnp.bfloat16),
        pltpu.VMEM((count, dets * rows * 2 + SUB, basis), jnp.bfloat16),
        pltpu.VMEM((count, dets, rows * 2, block // 2), CODE),
        pltpu.VMEM((count, dets, rows * 2, block // 2), CODE),
        pltpu.VMEM((dets, total + SLIDE_BLOCKS * wins, rows, WIN), jnp.float32),
        pltpu.VMEM((total // WIN * SUB, 1, WIN), jnp.float32),
        pltpu.VMEM((count, 1, WIN), jnp.float32),
    ]
    held = sum(math.prod(x.shape) * jnp.dtype(x.dtype).itemsize for x in scratch[1:-2])
    held += (count + total // WIN * SUB) * SUB * WIN * 4 + (4 << 20)
    extra = total * rows * WIN * 8
    adder = cores - 1 if held + extra <= VMEM_MOST and cores > 1 else None
    tiles = total if adder is not None else 2 * SUMS
    scratch += [
        pltpu.VMEM((tiles // 2, rows * 2, WIN), CODE),
        pltpu.VMEM((tiles // 2, rows * 2, WIN), CODE),
        pltpu.VMEM((tiles, rows, WIN), jnp.float32),
    ]
    held += tiles * rows * WIN * 8
    out = pl.pallas_call(
        functools.partial(kernel, chips, cores, adder),
        out_shape=jax.ShapeDtypeStruct((wins, count * rows), jnp.float32),
        in_specs=[hbm, hbm, hbm],
        out_specs=pl.BlockSpec(memory_space=pltpu.VMEM),
        scratch_shapes=scratch + [
            pltpu.SemaphoreType.DMA((3,)),
            pltpu.SemaphoreType.DMA((4,)),
            pltpu.SemaphoreType.DMA((count,)),
            pltpu.SemaphoreType.DMA((count,)),
            pltpu.SemaphoreType.DMA((1,)),
            pltpu.SemaphoreType.DMA((tiles // 2 // SUMS,)),
        ],
        compiler_params=pltpu.CompilerParams(
            collective_id=0, has_side_effects=True, vmem_limit_bytes=held),
    )(*(pltpu.with_memory_space_constraint(x, pltpu.HBM) for x in (offsets, basis_series, bank)))
    return out.T


def solution(mesh):
    chips, cores = mesh.shape["tmpl"], mesh.shape["det"]
    in_specs = (
        P(None, None, ("groups", "tmpl", "det")),
        P(None, ("groups", "tmpl"), None, None),
        P("groups"),
    )
    out_specs = P(None, ("groups", "tmpl", "det"))
    return jax.shard_map(
        functools.partial(per_device, chips, cores),
        mesh=mesh, in_specs=in_specs, out_specs=out_specs, check_vma=False,
    )
```

```python
import functools
import math

import jax
import jax.numpy as jnp
from jax import lax
from jax.experimental import pallas as pl
from jax.experimental.pallas import tpu as pltpu
from jax.sharding import PartitionSpec as P

WIN = 128
SUB = 8
SLIDE_BLOCKS = 16
SUMS = 32
VMEM_MOST = 62 << 20
MESH = pl.DeviceIdType.MESH
TINY = 1e-18
CODE = jnp.int16
SPAN = 30
STEPS = 1092
TOP = 15


def coded(power):
    log = jnp.log(jnp.maximum(power, 2.0 ** (TOP - 2 * SPAN))) * (STEPS / math.log(2.0))
    return jnp.round(log - (TOP - SPAN) * STEPS).astype(jnp.int32).astype(CODE)


def decoded(code):
    code = code.astype(jnp.int32).astype(jnp.float32)
    power = jnp.exp2(code * (1.0 / STEPS) + (TOP - SPAN))
    return jnp.where(code <= -SPAN * STEPS, 0.0, power)


def kernel(
    chips, cores, adder,
    off_hbm, basis_hbm, bank_hbm, out_ref,
    off_ref, basis_ref, bank_ref, bank_own, bank_all, stage, recv, dec, peaks, final,
    sums, added, part, load, sent, bank_r, pow_r, peak_r, sum_r,
):
    dets, basis, block = basis_ref.shape
    rows2 = bank_ref.shape[1] // cores
    rows = rows2 // 2
    half = block // 2
    wins = block // WIN
    count = chips * cores
    total = count * wins
    per_row = WIN // rows
    near = chips // 2
    chip, core = lax.axis_index("tmpl"), lax.axis_index("det")
    me = chip * cores + core
    side, place = lax.div(chip, near), lax.rem(chip, near)

    load_bank = pltpu.make_async_copy(bank_hbm, bank_ref, load.at[0])
    load_basis = pltpu.make_async_copy(basis_hbm, basis_ref, load.at[1])
    load_off = pltpu.make_async_copy(off_hbm, off_ref, load.at[2])
    load_bank.start()
    load_basis.start()
    load_off.start()

    def dev(j, c):
        return {"tmpl": j, "det": c}

    def across(j):
        return lax.rem(j + near, chips)

    def close(k):
        return side * near + lax.bitwise_xor(place, jnp.int32(k))

    def other_core(d):
        return lax.rem(core + d, cores)

    def over(lo, hi, fn, short=True):
        if short and hi - lo <= 8:
            for k in range(lo, hi):
                fn(k)
            return

        @pl.loop(lo, hi)
        def _(k):
            fn(k)

    def over_peers(fn):
        for d in range(cores):
            over(0, near, lambda k: fn(across(close(k)), other_core(d)))
        for d in range(cores):
            over(1, near, lambda k: fn(close(k), other_core(d)))
        for d in range(1, cores):
            fn(chip, other_core(d))

    barrier = pltpu.get_barrier_semaphore()
    over_peers(lambda j, c: pl.semaphore_signal(barrier, inc=1, device_id=dev(j, c), device_id_type=MESH))

    def bank_copy(j, src):
        return pltpu.make_async_remote_copy(
            src_ref=bank_all.at[src], dst_ref=bank_all.at[src], send_sem=sent.at[0], recv_sem=bank_r.at[src],
            device_id=dev(j, core), device_id_type=MESH)

    def pass_copy(src, c):
        return pltpu.make_async_remote_copy(
            src_ref=bank_all.at[src], dst_ref=bank_all.at[src],
            send_sem=sent.at[0], recv_sem=bank_r.at[src],
            device_id=dev(chip, c), device_id_type=MESH)

    def pow_copy(j, c, src):
        return pltpu.make_async_remote_copy(
            src_ref=stage.at[j * cores + c], dst_ref=recv.at[src],
            send_sem=sent.at[1], recv_sem=pow_r.at[src],
            device_id=dev(j, c), device_id_type=MESH)

    def over_all(ref, sem, n):
        some = ref.at[pl.ds(0, n)]
        return pltpu.make_async_remote_copy(
            src_ref=some, dst_ref=some, send_sem=sem, recv_sem=sem, device_id=dev(chip, core), device_id_type=MESH)

    def lift(i):
        return lax.rem(i + near * cores, count)

    def add_copy(j, src):
        slot = across(j) * cores + adder
        return pltpu.make_async_remote_copy(
            src_ref=stage.at[slot], dst_ref=recv.at[lift(src)],
            send_sem=sent.at[1], recv_sem=pow_r.at[lift(src)],
            device_id=dev(j, adder), device_id_type=MESH)

    def sum_copy(q):
        some = pl.ds(q * SUMS, SUMS)
        return pltpu.make_async_remote_copy(
            src_ref=sums.at[some], dst_ref=added.at[some], send_sem=sent.at[3], recv_sem=sum_r.at[q],
            device_id=dev(across(chip), adder), device_id_type=MESH)

    def near_copy(j, c):
        e = 0 if adder is None else lax.div(c, jnp.int32(adder))
        slot = across(j) * cores + c
        src = lax.rem(me + e * near * cores, count)
        return pltpu.make_async_remote_copy(
            src_ref=stage.at[slot], dst_ref=recv.at[src],
            send_sem=sent.at[1], recv_sem=pow_r.at[src],
            device_id=dev(lax.rem(j + (1 - e) * near, chips), c), device_id_type=MESH)

    def cross(j, fn, own=False):
        if adder is not None:
            add = lambda: fn(add_copy(j, me))
            pl.when(core != adder)(add) if own else add()
        for c in range(cores):
            if c != adder:
                fn(pow_copy(across(j), c, me))

    def peak_row(j, c):
        i = j * cores + c
        return lax.div(i, per_row) * SUB + lax.rem(SUB - lax.rem(i, SUB), SUB)

    def peak_copy(j, c, src):
        return pltpu.make_async_remote_copy(
            src_ref=peaks.at[peak_row(j, c)], dst_ref=final.at[src],
            send_sem=sent.at[2], recv_sem=peak_r.at[0],
            device_id=dev(j, c), device_id_type=MESH)

    span = dets * rows2
    size = span * cores
    r = lax.broadcasted_iota(jnp.int32, (size, size), 0)
    i = lax.broadcasted_iota(jnp.int32, (size, size), 1)
    c_of = lax.div(r, span)
    d_of = lax.rem(lax.div(r, rows2), dets)
    k_of = lax.rem(lax.div(r, rows), 2)
    m_of = lax.rem(r, rows)
    perm = (i == (d_of * cores + c_of) * rows2 + m_of * 2 + k_of).astype(jnp.float32).astype(jnp.bfloat16)

    def largest(x):
        x = jnp.abs(x).astype(jnp.float32)
        x = jnp.max(x.reshape(-1, SUB, x.shape[-1]), axis=0)
        return jnp.max(jnp.max(x, axis=0, keepdims=True), axis=1, keepdims=True)

    load_bank.wait()
    sorted_bank = jnp.dot(
        perm, bank_ref[...].reshape(size, basis), preferred_element_type=jnp.float32).astype(jnp.bfloat16)
    for c in range(cores):
        bank_own[c, :span] = sorted_bank[c * span:(c + 1) * span]
    load_basis.wait()
    first_rows = lax.broadcasted_iota(jnp.int32, (SUB, basis), 0) < SUB // 2
    top = largest(basis_ref[...].reshape(dets * basis, block))
    for c in range(cores):
        own_max = largest(sorted_bank[c * span:(c + 1) * span])
        note = jnp.where(first_rows, jnp.broadcast_to(top, (SUB, basis)), jnp.broadcast_to(own_max, (SUB, basis)))
        bank_own[c, span:] = note.astype(jnp.bfloat16)
    bank_all[me] = bank_own[core]

    def bank_max(bank, src):
        return bank[src, span:].astype(jnp.float32)[SUB // 2:SUB // 2 + 1, :1]

    def powers_for(j, bank, first):
        to = across(j)
        inv = []
        for c in range(cores):
            a = jnp.maximum(bank_max(bank, first + c) * top, TINY)
            inv.append(1.0 / (a * a))
        for d in range(dets):
            w = jnp.concatenate(
                [bank[first + c, d * rows2:(d + 1) * rows2] for c in range(cores)], axis=0)
            f = jnp.dot(w, basis_ref[d], preferred_element_type=jnp.float32)
            f = f * f
            for c in range(cores):
                p = (f[c * rows2:c * rows2 + rows] + f[c * rows2 + rows:(c + 1) * rows2]) * inv[c]
                stage[to * cores + c, d] = coded(jnp.concatenate([p[:, :half], p[:, half:]], axis=0))

    def pieces(j, fn):
        for d in range(1, cores):
            fn(j * cores + other_core(d))

    powers_for(chip, bank_own, 0)
    pl.semaphore_wait(barrier, count - 1)

    bank_copy(across(chip), me).start()
    over(1, near, lambda k: bank_copy(close(k), me).start())
    cross(chip, lambda copy: copy.start(), own=True)
    for d in range(1, cores):
        pass_copy(me, other_core(d)).start()

    def clear_edges():
        @pl.loop(0, count + SLIDE_BLOCKS)
        def _(n):
            for d in range(dets):
                dec[d, n * wins + wins - 1] = jnp.zeros((rows, WIN), jnp.float32)

    clear_edges()
    if adder is not None:
        @pl.when(core == adder)
        def _():
            dec[...] = jnp.zeros_like(dec)

        @pl.when(core != adder)
        def _():
            part[...] = jnp.zeros_like(part)


    def pass_on(src):
        bank_copy(chip, src).wait_recv()
        for d in range(1, cores):
            pass_copy(src, other_core(d)).start()

    def piece_powers(j, c):
        a = jnp.maximum(bank_max(bank_all, j * cores + c) * top, TINY)
        inv = 1.0 / (a * a)
        for d in range(dets):
            f = jnp.dot(
                bank_all[j * cores + c, d * rows2:(d + 1) * rows2], basis_ref[d], preferred_element_type=jnp.float32)
            f = f * f
            p = (f[:rows] + f[rows:]) * inv
            stage[across(j) * cores + c, d] = coded(jnp.concatenate([p[:, :half], p[:, half:]], axis=0))

    def near_direct(k, hold=False):
        pass_on(close(k) * cores + core)
        piece_powers(close(k), core)
        copy = near_copy(close(k), core)
        if not hold or adder is None:
            copy.start()
        else:
            pl.when(core == adder)(copy.start)

    def near_passed(k):
        for d in range(1, cores):
            bank_copy(chip, close(k) * cores + other_core(d)).wait_recv()
            piece_powers(close(k), other_core(d))
            near_copy(close(k), other_core(d)).start()

    near_direct(near // 2)
    relay = across(chip) * cores + core
    pass_on(relay)
    over(1, near, lambda k: bank_copy(close(k), relay).start())
    over(1, near // 2, lambda k: near_direct(near - k, True))
    over(1, near // 2, lambda k: near_direct(near // 2 - k, True))
    over(1, near, near_passed, short=False)

    def release(k):
        if adder is not None:
            pl.when(core != adder)(near_copy(close(k), core).start)

    over(1, near // 2, lambda k: release(near // 2 - k))
    over(1, near // 2, lambda k: release(near - k))

    over(1, near, lambda k: pass_on(across(close(k)) * cores + core))
    load_off.wait()
    rest = [lax.rem(off_ref[d], WIN) for d in range(dets)]
    shifts = [lax.div(off_ref[d], WIN) for d in range(dets)]
    lane = lax.broadcasted_iota(jnp.int32, (rows, WIN), 1)
    inside = [lane < WIN - rest[d] for d in range(dets)]

    def top_of(src):
        return bank_all[src, span:].astype(jnp.float32)[:1, :1]

    def scale_of(top, bank):
        a = jnp.maximum(top * bank, TINY)
        return a * a

    def kept(index, fn):
        fn(index)
        copied = lambda: fn(total + index)
        copied() if count <= SLIDE_BLOCKS else pl.when(index < SLIDE_BLOCKS * wins)(copied)

    def decode(src, value, bank):
        scale = scale_of(top_of(src), bank)
        first = src * wins
        before = lax.rem(first + total - 1, total)
        for d in range(dets):
            x = decoded(value(d)) * scale
            tiles = []
            for v in range(wins):
                h, q = divmod(v, wins // 2)
                tile = x[h * rows:(h + 1) * rows, q * WIN:(q + 1) * WIN]
                tiles.append(pltpu.roll(tile, WIN - rest[d], 1))
            head = jnp.where(inside[d], 0.0, tiles[0])
            tail = jnp.where(inside[d], tiles[-1], 0.0)

            def joined(at):
                for v in range(wins - 1):
                    dec[d, at + v] = jnp.where(inside[d], tiles[v], tiles[v + 1])
                dec[d, at + wins - 1] += tail

            def ahead(at):
                dec[d, at] += head

            kept(first, joined)
            kept(before, ahead)

    def adding(base):
        def leaf(v):
            power = None
            for d in range(dets):
                x = dec[d, base + shifts[d] + v]
                power = x if power is None else power + x
            return power

        return leaf

    def far_take():
        @pl.loop(0, near * cores)
        def _(n):
            src = across(close(lax.div(n, cores))) * cores + lax.rem(n, cores)
            pow_copy(chip, core, src).wait_recv()
            decode(src, lambda d: recv[src, d], owned)

    def add_near():
        bank = bank_max(bank_all, me)
        decode(me, lambda d: stage[lift(me), d], bank)

        def take(src):
            pow_copy(chip, core, lift(src)).wait_recv()
            decode(src, lambda d: recv[lift(src), d], bank)

        for d in range(1, cores):
            take(chip * cores + other_core(d))

        @pl.loop(cores, near * cores)
        def _(n):
            take(close(lax.div(n, cores)) * cores + lax.rem(n, cores))

        inv = 1.0 / (4.0 * scale_of(most(lambda k: close(k)), bank))

        @pl.loop(0, total // 2 // SUMS)
        def _(q):
            leaf = adding(q * 2 * SUMS)
            for v in range(SUMS):
                pair = jnp.concatenate([leaf(2 * v), leaf(2 * v + 1)], axis=0)
                sums[q * SUMS + v] = coded(pair * inv)
            sum_copy(q).start()

        clear_edges()

    def most(chip_of):
        tops = [bank_all[chip_of(k) * cores + c, span:] for k in range(near) for c in range(cores)]
        return functools.reduce(jnp.maximum, [x.astype(jnp.float32) for x in tops])[:1, :1]

    def take_sums():
        scale = 4.0 * scale_of(most(lambda k: across(close(k))), owned)

        @pl.loop(0, total // 2 // SUMS)
        def _(q):
            sum_copy(q).wait_recv()
            for v in range(SUMS):
                x = decoded(added[q * SUMS + v]) * scale
                part[(q * SUMS + v) * 2] = x[:rows]
                part[(q * SUMS + v) * 2 + 1] = x[rows:]

    pieces(chip, lambda src: bank_copy(chip, src).wait_recv())
    owned = bank_max(bank_all, across(chip) * cores + core)
    pieces(across(chip), lambda src: bank_copy(chip, src).wait_recv())
    powers_for(across(chip), bank_all, across(chip) * cores)
    for d in range(1, cores):
        pow_copy(chip, other_core(d), me).start()

    if adder is not None:
        pl.when(core == adder)(add_near)

    def far_powers(k):
        j = across(close(k))
        pieces(j, lambda src: bank_copy(chip, src).wait_recv())
        powers_for(j, bank_all, j * cores)
        for c in range(cores):
            pow_copy(close(k), c, me).start()

    over(1, near, lambda k: far_powers(near - k), short=False)

    if adder is None:
        far_take()
    else:
        pl.when(core != adder)(far_take)

    decode(me, lambda d: stage[me, d], owned)

    def take(j, c):
        src = j * cores + c
        pow_copy(chip, core, src).wait_recv()
        decode(src, lambda d: recv[src, d], owned)

    for d in range(1, cores):
        take(chip, other_core(d))

    @pl.loop(cores, near * cores)
    def _(n):
        take(close(lax.div(n, cores)), lax.rem(n, cores))

    if adder is not None:
        pl.when(core == adder)(take_sums)

    row = lax.broadcasted_iota(jnp.int32, (rows, WIN), 0)
    dest = lax.rem(SUB - row, SUB) + SUB * lax.div(lane, WIN // 2)
    index = SUB * lax.rem(dest + lax.rem(lane, SUB), per_row) + lax.rem(lax.div(lane, SUB), SUB)

    def group(g):
        base = g * WIN
        near_sum = adding(base)

        def leaf(v):
            return near_sum(v) if adder is None else near_sum(v) + part[base + v]

        x = jnp.zeros((rows, WIN), jnp.float32)
        for v in range(WIN):
            x = jnp.where(lane == v, jnp.max(leaf(v), axis=1, keepdims=True), x)
        x = jnp.sqrt(x)
        x = pltpu.roll(x, 0, 1, stride=SUB, stride_axis=0)
        for p in range(3):
            stay = lax.rem(lax.div(lane, SUB << p), 2) == 0
            x = jnp.where(stay, x, pltpu.roll(x, SUB - (1 << p), 0))
        x = jnp.take_along_axis(x, index, axis=1)
        for s in range(SUB):
            peaks[g * SUB + s] = x[s:s + 1]

    over(0, total // WIN, group, short=total == WIN)

    over_peers(lambda j, c: peak_copy(j, c, me).start())
    final[me] = peaks[peak_row(chip, core)]
    banks = near + (near - 1) + chips * (cores - 1)
    over_all(bank_all, sent.at[0], banks).wait_send()
    if adder is None:
        over_all(stage, sent.at[1], count - 1).wait_send()
    else:
        @pl.when(core == adder)
        def _():
            over_all(stage, sent.at[1], count - 2).wait_send()
            over_all(sums, sent.at[3], total // 2).wait_send()

        @pl.when(core != adder)
        def _():
            over_all(stage, sent.at[1], count - 1).wait_send()

    over_all(final, peak_r.at[0], count - 1).wait_recv()

    high = lax.rem(lax.div(me, SUB), 2) * (WIN // 2)
    e_of = lax.broadcasted_iota(jnp.int32, (per_row, WIN), 0)
    l_of = lax.broadcasted_iota(jnp.int32, (per_row, WIN), 1)
    groups = count // per_row
    for g in range(groups):
        to = (g + groups // 2) % groups if groups > 1 else 0
        x = final[g * per_row:(g + 1) * per_row].reshape(per_row, WIN)
        x = pltpu.roll(x, lax.rem(WIN - high, WIN), 1)
        turn = 0 if groups > 1 else per_row // 2
        x = jnp.concatenate([
            pltpu.roll(x[h:h + SUB], (h + turn) * rows % WIN, 1, stride=rows, stride_axis=0)
            for h in range(0, per_row, SUB)], axis=0)
        for i in range(wins):
            y = pltpu.roll(x, (WIN - i * rows) % WIN, 1)
            y = jnp.where(lax.div(l_of, rows) == lax.rem(e_of + turn, per_row), y, 0.0)
            out_ref[i:i + 1, to * WIN:(to + 1) * WIN] = jnp.sum(y, axis=0, keepdims=True)

    over_all(final, sent.at[2], count - 1).wait_send()


def per_device(chips, cores, basis_series, reconstruction, offsets):
    dets, basis, block = basis_series.shape
    templates = reconstruction.shape[1]
    bank = reconstruction.reshape(dets, templates * 2, basis)
    count = chips * cores
    rows = templates // cores
    wins = block // WIN
    total = count * wins
    hbm = pl.BlockSpec(memory_space=pltpu.HBM)
    scratch = [
        pltpu.SMEM(offsets.shape, offsets.dtype),
        pltpu.VMEM(basis_series.shape, basis_series.dtype),
        pltpu.VMEM(bank.shape, bank.dtype),
        pltpu.VMEM((cores, dets * rows * 2 + SUB, basis), jnp.bfloat16),
        pltpu.VMEM((count, dets * rows * 2 + SUB, basis), jnp.bfloat16),
        pltpu.VMEM((count, dets, rows * 2, block // 2), CODE),
        pltpu.VMEM((count, dets, rows * 2, block // 2), CODE),
        pltpu.VMEM((dets, total + SLIDE_BLOCKS * wins, rows, WIN), jnp.float32),
        pltpu.VMEM((total // WIN * SUB, 1, WIN), jnp.float32),
        pltpu.VMEM((count, 1, WIN), jnp.float32),
    ]
    held = sum(math.prod(x.shape) * jnp.dtype(x.dtype).itemsize for x in scratch[1:-2])
    held += (count + total // WIN * SUB) * SUB * WIN * 4 + (4 << 20)
    extra = total * rows * WIN * 8
    adder = cores - 1 if held + extra <= VMEM_MOST and cores > 1 else None
    tiles = total if adder is not None else 2 * SUMS
    scratch += [
        pltpu.VMEM((tiles // 2, rows * 2, WIN), CODE),
        pltpu.VMEM((tiles // 2, rows * 2, WIN), CODE),
        pltpu.VMEM((tiles, rows, WIN), jnp.float32),
    ]
    held += tiles * rows * WIN * 8
    out = pl.pallas_call(
        functools.partial(kernel, chips, cores, adder),
        out_shape=jax.ShapeDtypeStruct((wins, count * rows), jnp.float32),
        in_specs=[hbm, hbm, hbm],
        out_specs=pl.BlockSpec(memory_space=pltpu.VMEM),
        scratch_shapes=scratch + [
            pltpu.SemaphoreType.DMA((3,)),
            pltpu.SemaphoreType.DMA((4,)),
            pltpu.SemaphoreType.DMA((count,)),
            pltpu.SemaphoreType.DMA((count,)),
            pltpu.SemaphoreType.DMA((1,)),
            pltpu.SemaphoreType.DMA((tiles // 2 // SUMS,)),
        ],
        compiler_params=pltpu.CompilerParams(
            collective_id=0, has_side_effects=True, vmem_limit_bytes=held),
    )(*(pltpu.with_memory_space_constraint(x, pltpu.HBM) for x in (offsets, basis_series, bank)))
    return out.T


def solution(mesh):
    chips, cores = mesh.shape["tmpl"], mesh.shape["det"]
    in_specs = (
        P(None, None, ("groups", "tmpl", "det")),
        P(None, ("groups", "tmpl"), None, None),
        P("groups"),
    )
    out_specs = P(None, ("groups", "tmpl", "det"))
    return jax.shard_map(
        functools.partial(per_device, chips, cores),
        mesh=mesh, in_specs=in_specs, out_specs=out_specs, check_vma=False,
    )
```
